8 devices in a mesh: dp: 1 (over z), yax: 2 (over y), xax: 4 (over x, core).
Axes of the slice: x: 2, y: 2, z: 1, core: 2. Of those that a mesh axis runs over, the one named last changes fastest.
Arguments:
- hidden: bfloat16 [256, 2048], P('dp', 'xax')
- cache_len: int32 [256], P('dp')
- k_cache: bfloat16 [256, 8192, 128], P(('dp', 'yax', 'xax'))
- v_cache: bfloat16 [256, 8192, 128], P(('dp', 'yax', 'xax'))
- g_attn: float32 [2048], P('xax')
- w_query: bfloat16 [2048, 2048], P('xax', 'yax')
- w_key: bfloat16 [2048, 128], P('xax')
- w_value: bfloat16 [2048, 128], P('xax')
- w_gate: bfloat16 [2048, 8192], P('xax', 'yax')
- w_up: bfloat16 [2048, 8192], P('xax', 'yax')
- w_out: bfloat16 [2048, 2048], P('yax', 'xax')
- w_down: bfloat16 [8192, 2048], P('yax', 'xax')
- g_final: float32 [2048], P('xax')
- embedding: bfloat16 [50304, 2048], P('yax', 'xax')
Outputs:
- output 1: bfloat16 [256, 128], P(('dp', 'yax', 'xax'))
- output 2: bfloat16 [256, 128], P(('dp', 'yax', 'xax'))
- output 3: float32 [256, 50304], P('dp', ('yax', 'xax'))
- output 4: float32 [256], P('dp')
All inputs are finite; a program needn't handle non-finite values.
Results may differ from the reference program's by a relative error of at most 0.00831507.
Values are sent between devices in bfloat16 or wider.
A program may use at most 1 GiB of HBM per device.

```python
import jax
import jax.numpy as jnp
from jax import lax

D = 2048
HEADS = 16
HEAD = 128
FF = 8192
VOCAB = 50304
BATCH = 256
SEQ = 8192
ROW_BLOCK = 16

EPS = 1e-6
ROPE_BASE = 10000.0


def draw_lengths(key):
    drawn = jax.random.randint(key, (BATCH,), 1, SEQ, dtype=jnp.int32)
    row_ids = jnp.arange(BATCH)
    return jnp.where(row_ids == 0, SEQ - 1, jnp.where(row_ids == 1, 1, drawn)).astype(jnp.int32)


def setup_inputs(seed: int = 0, part: int = 0) -> dict:
    base_key = jax.random.key(seed)
    shared = jax.random.split(base_key, 10)
    own = jax.random.split(jax.random.fold_in(base_key, part), 5)

    def weight(key, shape, fan_in, gain):
        return (gain * fan_in ** -0.5 * jax.random.normal(key, shape, jnp.float32)).astype(jnp.bfloat16)

    col_scale = jnp.exp(0.5 * jax.random.normal(own[0], (D,), jnp.float32))
    hidden = jax.random.normal(own[1], (BATCH, D), jnp.float32) * col_scale
    k_cache = 2.5 * jax.random.normal(own[3], (BATCH, SEQ, HEAD), jnp.float32)
    v_cache = 2.0 * jax.random.normal(own[4], (BATCH, SEQ, HEAD), jnp.float32)
    return {
        "hidden": hidden.astype(jnp.bfloat16),
        "cache_len": draw_lengths(own[2]),
        "k_cache": k_cache.astype(jnp.bfloat16),
        "v_cache": v_cache.astype(jnp.bfloat16),
        "g_attn": 1.0 + 0.3 * jax.random.normal(shared[0], (D,), jnp.float32),
        "w_query": weight(shared[1], (D, HEADS * HEAD), D, 1.0),
        "w_key": weight(shared[2], (D, HEAD), D, 1.0),
        "w_value": weight(shared[3], (D, HEAD), D, 1.0),
        "w_gate": weight(shared[4], (D, FF), D, 1.0),
        "w_up": weight(shared[5], (D, FF), D, 1.0),
        "w_out": weight(shared[6], (HEADS * HEAD, D), HEADS * HEAD, 1.0),
        "w_down": weight(shared[7], (FF, D), FF, 1.0),
        "g_final": 1.0 + 0.3 * jax.random.normal(shared[8], (D,), jnp.float32),
        "embedding": weight(shared[9], (VOCAB, D), D, 2.0),
    }


def layer_norm(values_in, gain):
    row_mean = jnp.mean(values_in, axis=-1, keepdims=True)
    row_var = jnp.mean(jnp.square(values_in - row_mean), axis=-1, keepdims=True)
    return (values_in - row_mean) * lax.rsqrt(row_var + EPS) * gain


def rope_angle(positions):
    half_dim = HEAD // 2
    inv_freq = ROPE_BASE ** (-(jnp.arange(half_dim, dtype=jnp.float32) * 2.0) / HEAD)
    return positions.astype(jnp.float32)[:, None] * inv_freq[None, :]


def rotary(values_in, angles):
    half_dim = values_in.shape[-1] // 2
    cos_a = jnp.cos(angles)
    sin_a = jnp.sin(angles)
    first = values_in[..., :half_dim]
    second = values_in[..., half_dim:]
    return jnp.concatenate([first * cos_a - second * sin_a, second * cos_a + first * sin_a], axis=-1)


def attend_block(block):
    q_blk, kc_blk, vc_blk, kn_blk, vn_blk, len_blk = block
    positions = jnp.arange(SEQ)
    at_slot = positions[None, :, None] == len_blk[:, None, None]
    keys_all = jnp.where(at_slot, kn_blk[:, None, :], kc_blk)
    values_all = jnp.where(at_slot, vn_blk[:, None, :], vc_blk)
    scores = jnp.einsum("rhe,rse->rhs", q_blk.astype(jnp.float32), keys_all.astype(jnp.float32)) * HEAD ** -0.5
    valid = positions[None, None, :] <= len_blk[:, None, None]
    scores = jnp.where(valid, scores, -jnp.inf)
    prob_all = jax.nn.softmax(scores, axis=-1).astype(jnp.bfloat16)
    mixed = jnp.einsum("rhs,rse->rhe", prob_all.astype(jnp.float32), values_all.astype(jnp.float32))
    return mixed.astype(jnp.bfloat16)


def reference(hidden, cache_len, k_cache, v_cache, g_attn, w_query, w_key, w_value,
              w_gate, w_up, w_out, w_down, g_final, embedding):
    residual = hidden.astype(jnp.float32)
    normed = layer_norm(residual, g_attn).astype(jnp.bfloat16)
    query = jnp.dot(normed, w_query, preferred_element_type=jnp.float32).astype(jnp.bfloat16)
    key_new = jnp.dot(normed, w_key, preferred_element_type=jnp.float32).astype(jnp.bfloat16)
    value_new = jnp.dot(normed, w_value, preferred_element_type=jnp.float32).astype(jnp.bfloat16)
    gate = jnp.dot(normed, w_gate, preferred_element_type=jnp.float32).astype(jnp.bfloat16)
    up_val = jnp.dot(normed, w_up, preferred_element_type=jnp.float32).astype(jnp.bfloat16)
    angles = rope_angle(cache_len)
    query = rotary(query.astype(jnp.float32).reshape(BATCH, HEADS, HEAD), angles[:, None, :]).astype(jnp.bfloat16)
    key_new = rotary(key_new.astype(jnp.float32), angles).astype(jnp.bfloat16)
    blocks = BATCH // ROW_BLOCK
    attn_out = lax.map(attend_block, (
        query.reshape(blocks, ROW_BLOCK, HEADS, HEAD),
        k_cache.reshape(blocks, ROW_BLOCK, SEQ, HEAD),
        v_cache.reshape(blocks, ROW_BLOCK, SEQ, HEAD),
        key_new.reshape(blocks, ROW_BLOCK, HEAD),
        value_new.reshape(blocks, ROW_BLOCK, HEAD),
        cache_len.reshape(blocks, ROW_BLOCK)))
    attn_out = attn_out.reshape(BATCH, HEADS * HEAD)
    mlp_act = (jax.nn.silu(gate.astype(jnp.float32)) * up_val.astype(jnp.float32)).astype(jnp.bfloat16)
    branch_sum = (jnp.dot(attn_out, w_out, preferred_element_type=jnp.float32)
                  + jnp.dot(mlp_act, w_down, preferred_element_type=jnp.float32))
    residual_out = residual + branch_sum
    final_norm = layer_norm(residual_out, g_final).astype(jnp.bfloat16)
    logits = jnp.dot(final_norm, embedding.T, preferred_element_type=jnp.float32)
    log_norm = jax.nn.logsumexp(logits, axis=-1)
    return key_new, value_new, logits - log_norm[:, None], log_norm
```

```python
import functools

import jax
import jax.numpy as jnp
from jax import lax
from jax.experimental import pallas as pl
from jax.experimental.pallas import tpu as pltpu
from jax.sharding import PartitionSpec as P

EPS = 1e-6
ROPE_BASE = 10000.0


def rope_angle(positions, head_dim):
    half_dim = head_dim // 2
    inv_freq = ROPE_BASE ** (-(jnp.arange(half_dim, dtype=jnp.float32) * 2.0) / head_dim)
    return positions.astype(jnp.float32)[:, None] * inv_freq[None, :]


def rotary(values_in, angles):
    half_dim = values_in.shape[-1] // 2
    cos_a = jnp.cos(angles)
    sin_a = jnp.sin(angles)
    first = values_in[..., :half_dim]
    second = values_in[..., half_dim:]
    return jnp.concatenate([first * cos_a - second * sin_a, second * cos_a + first * sin_a], axis=-1)


def sharded_norm(values_in, gain, width):
    stats = jnp.stack([jnp.sum(values_in, axis=-1), jnp.sum(values_in * values_in, axis=-1)])
    stats = lax.psum(stats, "xax")
    row_mean = stats[0] / width
    row_var = stats[1] / width - row_mean * row_mean
    return (values_in - row_mean[:, None]) * lax.rsqrt(row_var + EPS)[:, None] * gain


def attend_local(query, k_cache, v_cache, key_new, value_new, lengths):
    score_scale = query.shape[-1] ** -0.5
    scores = jnp.einsum("bhe,bse->bhs", query, k_cache, preferred_element_type=jnp.float32) * score_scale
    score_new = jnp.einsum("bhe,be->bh", query, key_new, preferred_element_type=jnp.float32) * score_scale
    valid = jnp.arange(k_cache.shape[1])[None, None, :] < lengths[:, None, None]
    row_max = jnp.maximum(jnp.max(jnp.where(valid, scores, -jnp.inf), axis=-1), score_new)
    weights = jnp.where(valid, jnp.exp(scores - row_max[..., None]), 0.0)
    weight_new = jnp.exp(score_new - row_max)
    denominator = jnp.sum(weights, axis=-1) + weight_new
    prob_all = (weights / denominator[..., None]).astype(jnp.bfloat16)
    prob_new = (weight_new / denominator).astype(jnp.bfloat16)
    attn_out = jnp.einsum("bhs,bse->bhe", prob_all, v_cache, preferred_element_type=jnp.float32)
    attn_out = attn_out + prob_new.astype(jnp.float32)[..., None] * value_new.astype(jnp.float32)[:, None, :]
    return attn_out.astype(jnp.bfloat16)


MESH = pl.DeviceIdType.MESH
V_TILE = 512
NT_DIMS = (((1,), (1,)), ((), ()))


def positions(x_size):
    y_idx = lax.axis_index("yax")
    d_idx = lax.axis_index("xax")
    core = lax.rem(d_idx, 2)
    chip = d_idx // 2
    return y_idx, d_idx, core, chip


def all_barrier(y_size, x_size, y_idx, d_idx):
    barrier = pltpu.get_barrier_semaphore()
    for step in range(1, y_size * x_size):
        flat = lax.rem(y_idx * x_size + d_idx + step, y_size * x_size)
        pl.semaphore_signal(barrier, inc=1, device_id={"yax": flat // x_size, "xax": lax.rem(flat, x_size)},
                            device_id_type=MESH)
    pl.semaphore_wait(barrier, y_size * x_size - 1)


def head_kernel(y_size, x_size, f_ref, emb_ref, out_ref, norm_ref, ebuf, f_peer, send, recv, out_buf,
                stat_own, stat_all, own_sem, peer_ssem, peer_rsem, f_ssem, f_rsem, z_ssem, z_rsem,
                stat_ssem, stat_rsem, out_sem):
    y_idx, d_idx, core, chip = positions(x_size)
    partner = 2 * chip + (1 - core)
    x_nbr = 2 * (1 - chip) + core
    n_dev = y_size * x_size
    flat = y_idx * x_size + d_idx
    v_quarter = recv.shape[1]
    half_rows = recv.shape[2]
    chunks = recv.shape[0]
    full_tiles = v_quarter // V_TILE
    tail = v_quarter - full_tiles * V_TILE
    n_tiles = full_tiles + 1

    def tile_span(idx):
        return (V_TILE if idx != full_tiles else tail)

    def e_own_copy(quarter, tile, size):
        place = 2 * (1 - chip) + core if quarter == 0 else d_idx
        start = pl.multiple_of(place * v_quarter + tile * V_TILE, 16)
        off = pl.multiple_of(tile * V_TILE, V_TILE)
        return pltpu.make_async_copy(emb_ref.at[pl.ds(start, size), :], ebuf.at[0, quarter, pl.ds(off, size), :],
                                     own_sem.at[quarter, tile])

    def e_peer_copy(quarter, tile, size):
        place = 2 * (1 - chip) + (1 - core) if quarter == 0 else partner
        start = pl.multiple_of(place * v_quarter + tile * V_TILE, 16)
        off = pl.multiple_of(tile * V_TILE, V_TILE)
        return pltpu.make_async_remote_copy(
            src_ref=emb_ref.at[pl.ds(start, size), :], dst_ref=ebuf.at[1, quarter, pl.ds(off, size), :],
            send_sem=peer_ssem.at[quarter, tile], recv_sem=peer_rsem.at[quarter, tile],
            device_id={"xax": partner}, device_id_type=MESH)

    def z_copy(chunk, tile, size):
        off = pl.multiple_of(tile * V_TILE, V_TILE)
        return pltpu.make_async_remote_copy(
            src_ref=send.at[chunk, pl.ds(off, size), :], dst_ref=recv.at[chunk, pl.ds(off, size), :],
            send_sem=z_ssem.at[chunk, tile], recv_sem=z_rsem.at[chunk, tile],
            device_id={"xax": x_nbr}, device_id_type=MESH)

    def f_copy(chunk):
        rows = pl.ds(chunk * half_rows, half_rows)
        return pltpu.make_async_remote_copy(
            src_ref=f_ref.at[rows, :], dst_ref=f_peer.at[chunk], send_sem=f_ssem.at[chunk],
            recv_sem=f_rsem.at[chunk], device_id={"xax": partner}, device_id_type=MESH)

    def over_tiles(body):
        @pl.loop(0, full_tiles)
        def _(tile):
            body(tile, V_TILE)
        body(full_tiles, tail)

    @pl.loop(0, full_tiles)
    def _(tile):
        e_own_copy(0, tile, V_TILE).start()
    e_own_copy(0, full_tiles, tail).start()
    all_barrier(y_size, x_size, y_idx, d_idx)
    for chunk in range(chunks):
        f_copy(chunk).start()
    over_tiles(lambda tile, size: e_peer_copy(0, tile, size).start())
    over_tiles(lambda tile, size: e_own_copy(1, tile, size).start())
    over_tiles(lambda tile, size: e_peer_copy(1, tile, size).start())

    def partial(chunk, quarter, tile, size):
        off = pl.multiple_of(tile * V_TILE, V_TILE)
        f_own = f_ref[pl.ds(chunk * half_rows, half_rows), :]
        return (lax.dot_general(ebuf[0, quarter, pl.ds(off, size), :], f_own, NT_DIMS,
                                preferred_element_type=jnp.float32)
                + lax.dot_general(ebuf[1, quarter, pl.ds(off, size), :], f_peer[chunk], NT_DIMS,
                                  preferred_element_type=jnp.float32))

    def send_chunk(chunk):
        def one(tile, size):
            if chunk == 0:
                e_own_copy(0, tile, size).wait()
                e_peer_copy(0, tile, size).wait_recv()
            off = pl.multiple_of(tile * V_TILE, V_TILE)
            send[chunk, pl.ds(off, size), :] = partial(chunk, 0, tile, size)

        @pl.loop(0, full_tiles)
        def _(tile):
            one(tile, V_TILE)

            @pl.when(tile > 0)
            def _():
                z_copy(chunk, tile - 1, V_TILE).start()
        one(full_tiles, tail)
        z_copy(chunk, full_tiles - 1, V_TILE).start()
        z_copy(chunk, full_tiles, tail).start()

    for chunk in range(chunks):
        f_copy(chunk).wait_recv()
        send_chunk(chunk)

    def take_tile(chunk, tile, size, carry):
        run_max, run_sum = carry
        off = pl.multiple_of(tile * V_TILE, V_TILE)
        if chunk == 0:
            e_own_copy(1, tile, size).wait()
            e_peer_copy(1, tile, size).wait_recv()
        own = partial(chunk, 1, tile, size)
        z_copy(chunk, tile, size).wait_recv()
        z_val = own + recv[chunk, pl.ds(off, size), :]
        recv[chunk, pl.ds(off, size), :] = z_val
        z_grp = z_val.reshape(size // 8, 8, half_rows)
        new_max = jnp.maximum(run_max, jnp.max(z_grp, axis=0))
        new_sum = run_sum * jnp.exp(run_max - new_max) + jnp.sum(jnp.exp(z_grp - new_max[None]), axis=0)
        return new_max, new_sum

    def stat_copy(chunk, step):
        other = lax.rem(flat + step, n_dev)
        return pltpu.make_async_remote_copy(
            src_ref=stat_own.at[chunk], dst_ref=stat_all.at[chunk, flat], send_sem=stat_ssem.at[chunk, step],
            recv_sem=stat_rsem.at[chunk, step],
            device_id={"yax": other // x_size, "xax": lax.rem(other, x_size)}, device_id_type=MESH)

    def out_copy(chunk):
        return pltpu.make_async_copy(out_buf.at[chunk], out_ref.at[pl.ds(chunk * half_rows, half_rows), :],
                                     out_sem.at[chunk])

    def finish_chunk(chunk):
        low = jnp.full((8, half_rows), -jnp.inf, jnp.float32)
        carry = take_tile(chunk, 0, V_TILE, (low, jnp.zeros((8, half_rows), jnp.float32)))
        carry = lax.fori_loop(1, full_tiles, lambda tile, c: take_tile(chunk, tile, V_TILE, c), carry)
        run_max, run_sum = take_tile(chunk, full_tiles, tail, carry)
        top = jnp.max(run_max, axis=0, keepdims=True)
        total = jnp.sum(run_sum * jnp.exp(run_max - top), axis=0, keepdims=True)
        sub = lax.broadcasted_iota(jnp.int32, (8, half_rows), 0)
        both = jnp.where(sub == 0, top, total)
        stat_own[chunk] = both
        stat_all[chunk, flat] = both
        for step in range(1, n_dev):
            stat_copy(chunk, step).start()
        for step in range(1, n_dev):
            stat_copy(chunk, step).wait_recv()
        tops = [stat_all[chunk, i, 0:1, :] for i in range(n_dev)]
        top_all = tops[0]
        for item in tops[1:]:
            top_all = jnp.maximum(top_all, item)
        sum_all = jnp.zeros_like(top_all)
        for i in range(n_dev):
            sum_all = sum_all + stat_all[chunk, i, 1:2, :] * jnp.exp(tops[i] - top_all)
        log_norm = top_all + jnp.log(sum_all)
        norm_ref[:, pl.ds(chunk * half_rows, half_rows)] = log_norm

        lanes = v_quarter // 128

        @pl.loop(0, lanes)
        def _(blk):
            off = pl.multiple_of(blk * 128, 128)
            out_buf[chunk, :, pl.ds(off, 128)] = jnp.transpose(recv[chunk, pl.ds(off, 128), :] - log_norm)
        left = v_quarter - lanes * 128
        if left:
            out_buf[chunk, :, pl.ds(lanes * 128, left)] = jnp.transpose(
                recv[chunk, pl.ds(lanes * 128, left), :] - log_norm)
        out_copy(chunk).start()

    for chunk in range(chunks):
        finish_chunk(chunk)

    for chunk in range(chunks):
        out_copy(chunk).wait()
        f_copy(chunk).wait_send()
        over_tiles(lambda tile, size: z_copy(chunk, tile, size).wait_send())
        over_tiles(lambda tile, size: e_peer_copy(chunk, tile, size).wait_send())
        for step in range(1, n_dev):
            stat_copy(chunk, step).wait_send()


def head_call(mesh, final_norm, embedding):
    y_size, x_size = mesh.shape["yax"], mesh.shape["xax"]
    rows, width = final_norm.shape
    v_quarter = embedding.shape[0] // x_size
    half = rows // 2
    tiles = v_quarter // V_TILE + 1
    n_dev = y_size * x_size
    dma = pltpu.SemaphoreType.DMA
    vm = pltpu.VMEM
    any_spec = pl.BlockSpec(memory_space=pl.ANY)
    vmem_spec = pl.BlockSpec(memory_space=pltpu.VMEM)
    return pl.pallas_call(
        functools.partial(head_kernel, y_size, x_size),
        out_shape=(jax.ShapeDtypeStruct((rows, v_quarter), jnp.float32),
                   jax.ShapeDtypeStruct((1, rows), jnp.float32)),
        in_specs=[vmem_spec, any_spec],
        out_specs=(any_spec, vmem_spec),
        scratch_shapes=[
            vm((2, 2, v_quarter, width), jnp.bfloat16), vm((2, half, width), jnp.bfloat16),
            vm((2, v_quarter, half), jnp.float32), vm((2, v_quarter, half), jnp.float32),
            vm((2, half, v_quarter), jnp.float32),
            vm((2, 8, half), jnp.float32), vm((2, n_dev, 8, half), jnp.float32),
            dma((2, tiles)), dma((2, tiles)), dma((2, tiles)), dma((2,)), dma((2,)), dma((2, tiles)), dma((2, tiles)),
            dma((2, n_dev)), dma((2, n_dev)), dma((2,))],
        compiler_params=pltpu.CompilerParams(collective_id=0, has_side_effects=True, vmem_limit_bytes=62 * 1024 * 1024),
        cost_estimate=pl.CostEstimate(flops=2 * rows * 2 * v_quarter * 2 * width, bytes_accessed=40_000_000,
                                      transcendentals=rows * v_quarter),
        name="head",
    )(final_norm, embedding)


def solution(mesh):
    y_size = mesh.shape["yax"]
    x_size = mesh.shape["xax"]
    row_spec = P(("dp", "yax", "xax"))

    def local_step(hidden, cache_len, k_cache, v_cache, g_attn, w_query, w_key, w_value,
                   w_gate, w_up, w_out, w_down, g_final, embedding):
        rows = hidden.shape[0]
        width = hidden.shape[1] * x_size
        own_rows = k_cache.shape[0]
        head_dim = k_cache.shape[2]
        q_cols = w_query.shape[1]
        kv_end = q_cols + 2 * head_dim
        ff_end = kv_end + w_gate.shape[1]
        y_idx = lax.axis_index("yax")
        x_idx = lax.axis_index("xax")
        own_start = (y_idx * x_size + x_idx) * own_rows

        residual = hidden.astype(jnp.float32)
        normed = sharded_norm(residual, g_attn, width).astype(jnp.bfloat16)
        proj_part = jnp.concatenate([
            jnp.dot(normed, w_query, preferred_element_type=jnp.float32),
            jnp.dot(normed, w_key, preferred_element_type=jnp.float32),
            jnp.dot(normed, w_value, preferred_element_type=jnp.float32),
            jnp.dot(normed, w_gate, preferred_element_type=jnp.float32),
            jnp.dot(normed, w_up, preferred_element_type=jnp.float32)], axis=1)
        projected = lax.psum(proj_part, "xax").astype(jnp.bfloat16)
        angles = rope_angle(cache_len, head_dim)
        query = projected[:, :q_cols].astype(jnp.float32).reshape(rows, q_cols // head_dim, head_dim)
        query = rotary(query, angles[:, None, :]).astype(jnp.bfloat16)
        key_new = rotary(projected[:, q_cols:q_cols + head_dim].astype(jnp.float32), angles).astype(jnp.bfloat16)
        value_new = projected[:, q_cols + head_dim:kv_end]
        gate = projected[:, kv_end:ff_end]
        up_val = projected[:, ff_end:]

        query_grp = lax.all_to_all(query, "yax", 0, 1, tiled=True)
        query_own = lax.dynamic_slice_in_dim(query_grp, x_idx * own_rows, own_rows, axis=0)
        key_own = lax.dynamic_slice_in_dim(key_new, own_start, own_rows, axis=0)
        value_own = lax.dynamic_slice_in_dim(value_new, own_start, own_rows, axis=0)
        len_own = lax.dynamic_slice_in_dim(cache_len, own_start, own_rows, axis=0)
        attn_own = attend_local(query_own, k_cache, v_cache, key_own, value_own, len_own)
        attn_grp = lax.all_gather(attn_own, "xax", axis=0, tiled=True)
        attn_heads = lax.all_to_all(attn_grp, "yax", 1, 0, tiled=True).reshape(rows, q_cols)

        mlp_act = (jax.nn.silu(gate.astype(jnp.float32)) * up_val.astype(jnp.float32)).astype(jnp.bfloat16)
        branch_sum = (jnp.dot(attn_heads, w_out, preferred_element_type=jnp.float32)
                      + jnp.dot(mlp_act, w_down, preferred_element_type=jnp.float32))
        residual_out = residual + lax.psum(branch_sum, "yax")
        final_norm = sharded_norm(residual_out, g_final, width).astype(jnp.bfloat16)
        log_probs, log_norm = head_call(mesh, final_norm, embedding)
        return key_own, value_own, log_probs, log_norm.reshape(rows)

    in_specs = (P("dp", "xax"), P("dp"), row_spec, row_spec, P("xax"), P("xax", "yax"),
                P("xax", None), P("xax", None), P("xax", "yax"), P("xax", "yax"),
                P("yax", "xax"), P("yax", "xax"), P("xax"), P("yax", "xax"))
    out_specs = (row_spec, row_spec, P("dp", ("yax", "xax")), P("dp"))
    return jax.shard_map(local_step, mesh=mesh, in_specs=in_specs, out_specs=out_specs, check_vma=False)
```

```python
import functools

import jax
import jax.numpy as jnp
from jax import lax
from jax.experimental import pallas as pl
from jax.experimental.pallas import tpu as pltpu
from jax.sharding import PartitionSpec as P

EPS = 1e-6
ROPE_BASE = 10000.0


def rope_angle(positions, head_dim):
    half_dim = head_dim // 2
    inv_freq = ROPE_BASE ** (-(jnp.arange(half_dim, dtype=jnp.float32) * 2.0) / head_dim)
    return positions.astype(jnp.float32)[:, None] * inv_freq[None, :]


MESH = pl.DeviceIdType.MESH
V_TILE = 512
NT_DIMS = (((1,), (1,)), ((), ()))


def positions(x_size):
    y_idx = lax.axis_index("yax")
    d_idx = lax.axis_index("xax")
    core = lax.rem(d_idx, 2)
    chip = d_idx // 2
    return y_idx, d_idx, core, chip


def all_barrier(y_size, x_size, y_idx, d_idx):
    barrier = pltpu.get_barrier_semaphore()
    for step in range(1, y_size * x_size):
        flat = lax.rem(y_idx * x_size + d_idx + step, y_size * x_size)
        pl.semaphore_signal(barrier, inc=1, device_id={"yax": flat // x_size, "xax": lax.rem(flat, x_size)},
                            device_id_type=MESH)
    pl.semaphore_wait(barrier, y_size * x_size - 1)


def compact_rows(first, second):
    rows = first.shape[0]
    lane = lax.broadcasted_iota(jnp.int32, (rows, 128), 1)
    return jnp.transpose(jnp.where(lane == 0, first, second))[0:8, :]


def spread_rows(first, second):
    rows = first.shape[1]
    sub = lax.broadcasted_iota(jnp.int32, (128, rows), 0)
    cols = jnp.transpose(jnp.where(sub == 0, first, second))
    return cols[:, 0:1], cols[:, 1:2]


def local_moments(values_in):
    part = values_in.shape[1]
    mean = jnp.sum(values_in, axis=1, keepdims=True) / part
    diff = values_in - mean
    return mean, jnp.sum(diff * diff, axis=1, keepdims=True)


def join_moments(stats, count, part):
    mean = stats[0][0:1, :]
    for item in stats[1:]:
        mean = mean + item[0:1, :]
    mean = mean / count
    square = jnp.zeros_like(mean)
    for item in stats:
        shift = item[0:1, :] - mean
        square = square + item[1:2, :] + part * shift * shift
    return mean, lax.rsqrt(square / (count * part) + EPS)


def project_kernel(y_size, x_size, hid_ref, gain_ref, cos_ref, sin_ref, wq_ref, wk_ref, wv_ref, wg_ref, wu_ref,
                   q_out, k_out, v_out, keep_out, send_a_out, send_b_out,
                   hid_peer, gain_peer, wq_buf, wkv_buf, wgu_buf, n_buf, stat_own, stat_all,
                   q_send, q_recv, kv_send, kv_recv, q_bf, q_peer, gu_buf,
                   hid_sem, stat_ssem, stat_rsem, wl_sem, wp_ssem, wp_rsem, q_sem, y_sem, out_sem):
    y_idx, d_idx, core, chip = positions(x_size)
    partner = 2 * chip + (1 - core)
    x_nbr = 2 * (1 - chip) + core
    rows, part = hid_ref.shape
    half = rows // 2
    own_rows = q_out.shape[0]
    q_cols = wq_ref.shape[1]
    head_dim = wk_ref.shape[1]
    ff_cols = wgu_buf.shape[3] // 2
    n_blk = rows // own_rows

    def ff_block(j, which_core):
        place = (2 * (1 - chip) if j == 0 else 2 * chip) + which_core
        return pl.ds(pl.multiple_of(place * ff_cols, 128), ff_cols)

    def small_dsts(side):
        return (wq_buf.at[side], wkv_buf.at[side, :, pl.ds(0, head_dim)], wkv_buf.at[side, :, pl.ds(head_dim, head_dim)])

    local = [pltpu.make_async_copy(src, dst, wl_sem.at[i])
             for i, (src, dst) in enumerate(zip((wq_ref, wk_ref, wv_ref), small_dsts(0)))]
    remote = [pltpu.make_async_remote_copy(src_ref=src, dst_ref=dst, send_sem=wp_ssem.at[i], recv_sem=wp_rsem.at[i],
                                           device_id={"xax": partner}, device_id_type=MESH)
              for i, (src, dst) in enumerate(zip((wq_ref, wk_ref, wv_ref), small_dsts(1)))]
    local_gu, remote_gu = [], []
    for j in range(2):
        for which, src in enumerate((wg_ref, wu_ref)):
            i = 3 + 2 * j + which
            dst_cols = pl.ds(which * ff_cols, ff_cols)
            local_gu.append(pltpu.make_async_copy(src.at[:, ff_block(j, core)], wgu_buf.at[0, j, :, dst_cols],
                                                  wl_sem.at[i]))
            remote_gu.append(pltpu.make_async_remote_copy(
                src_ref=src.at[:, ff_block(j, 1 - core)], dst_ref=wgu_buf.at[1, j, :, dst_cols],
                send_sem=wp_ssem.at[i], recv_sem=wp_rsem.at[i], device_id={"xax": partner}, device_id_type=MESH))
    hid_copy = pltpu.make_async_remote_copy(src_ref=hid_ref, dst_ref=hid_peer, send_sem=hid_sem.at[0],
                                            recv_sem=hid_sem.at[1], device_id={"xax": partner}, device_id_type=MESH)
    gain_copy = pltpu.make_async_remote_copy(src_ref=gain_ref, dst_ref=gain_peer, send_sem=hid_sem.at[2],
                                             recv_sem=hid_sem.at[3], device_id={"xax": partner}, device_id_type=MESH)

    def stat_copy(step):
        return pltpu.make_async_remote_copy(
            src_ref=stat_own, dst_ref=stat_all.at[d_idx], send_sem=stat_ssem.at[step], recv_sem=stat_rsem.at[step],
            device_id={"xax": lax.rem(d_idx + step, x_size)}, device_id_type=MESH)

    for item in local:
        item.start()
    all_barrier(y_size, x_size, y_idx, d_idx)
    hid_copy.start()
    gain_copy.start()
    for item in remote:
        item.start()
    for item in local_gu:
        item.start()

    hid = hid_ref[...].astype(jnp.float32)
    mean_own, square_own = local_moments(hid)
    packed = compact_rows(mean_own, square_own)
    stat_own[...] = packed
    stat_all[d_idx] = packed
    for step in range(1, x_size):
        stat_copy(step).start()
    for item in remote_gu:
        item.start()
    hid_copy.wait_recv()
    gain_copy.wait_recv()
    for step in range(1, x_size):
        stat_copy(step).wait_recv()
    mean, rstd = spread_rows(*join_moments([stat_all[i] for i in range(x_size)], x_size, part))
    n_buf[0] = ((hid - mean) * rstd * gain_ref[0:1, :]).astype(jnp.bfloat16)
    n_buf[1] = ((hid_peer[...].astype(jnp.float32) - mean) * rstd * gain_peer[0:1, :]).astype(jnp.bfloat16)

    def dest_rows(y_at, chip_at):
        return pl.ds(pl.multiple_of(y_at * half + (2 * chip_at + core) * own_rows, own_rows), own_rows)

    def two_dots(row_sets, weights):
        left = [jnp.concatenate([n_buf[side, r, :] for r in row_sets], axis=0) if len(row_sets) > 1
                else n_buf[side, row_sets[0], :] for side in range(2)]
        return (jnp.dot(left[0], weights.at[0][...], preferred_element_type=jnp.float32)
                + jnp.dot(left[1], weights.at[1][...], preferred_element_type=jnp.float32))

    for item in local:
        item.wait()
    for item in remote:
        item.wait_recv()
    q_send[...] = two_dots([dest_rows(0, 1 - chip), dest_rows(1, 1 - chip)], wq_buf)
    kv_send[...] = two_dots([dest_rows(y_idx, 1 - chip)], wkv_buf)
    q_copy = pltpu.make_async_remote_copy(src_ref=q_send, dst_ref=q_recv, send_sem=q_sem.at[0], recv_sem=q_sem.at[1],
                                          device_id={"xax": x_nbr}, device_id_type=MESH)
    kv_copy = pltpu.make_async_remote_copy(src_ref=kv_send, dst_ref=kv_recv, send_sem=q_sem.at[2],
                                           recv_sem=q_sem.at[3], device_id={"xax": x_nbr}, device_id_type=MESH)
    q_copy.start()
    q_keep = two_dots([dest_rows(0, chip), dest_rows(1, chip)], wq_buf)
    kv_copy.start()
    kv_keep = two_dots([dest_rows(y_idx, chip)], wkv_buf)

    for item in local_gu:
        item.wait()
    for item in remote_gu:
        item.wait_recv()

    gu_outs = [[pltpu.make_async_copy(gu_buf.at[0, 0], send_a_out, out_sem.at[0]),
                pltpu.make_async_copy(gu_buf.at[0, 1], send_b_out, out_sem.at[1])],
               [pltpu.make_async_copy(gu_buf.at[1, r], keep_out.at[pl.ds(r * half, half), :], out_sem.at[2 + r])
                for r in range(2)]]

    def gu_part(j, r):
        span = pl.ds(r * half, half)

        @pl.loop(0, 2 * ff_cols // 512)
        def _(t):
            cols = pl.ds(pl.multiple_of(t * 512, 512), 512)
            gu_buf[j, r, :, cols] = (
                jnp.dot(n_buf[0, span, :], wgu_buf[0, j, :, cols], preferred_element_type=jnp.float32)
                + jnp.dot(n_buf[1, span, :], wgu_buf[1, j, :, cols], preferred_element_type=jnp.float32))

    for r in range(2):
        gu_part(0, r)
        gu_outs[0][r].start()

    def rotate(values_in):
        val = values_in.astype(jnp.float32)
        return (val * cos_ref[...] + pltpu.roll(val, head_dim // 2, 1) * sin_ref[...]).astype(jnp.bfloat16)

    q_copy.wait_recv()
    q_bf[...] = (q_keep + q_recv[...]).astype(jnp.bfloat16)
    y_copy = pltpu.make_async_remote_copy(
        src_ref=q_bf.at[pl.ds(pl.multiple_of((1 - y_idx) * own_rows, own_rows), own_rows), :], dst_ref=q_peer,
        send_sem=y_sem.at[0], recv_sem=y_sem.at[1], device_id={"yax": 1 - y_idx}, device_id_type=MESH)
    y_copy.start()
    kv_copy.wait_recv()
    kv_bf = (kv_keep + kv_recv[...]).astype(jnp.bfloat16)
    k_out[...] = rotate(kv_bf[:, :head_dim])
    v_out[...] = kv_bf[:, head_dim:]
    for r in range(2):
        gu_part(1, r)
        gu_outs[1][r].start()
    own_span = pl.ds(pl.multiple_of(y_idx * own_rows, own_rows), own_rows)
    for h in range(q_cols // head_dim):
        cols = pl.ds(h * head_dim, head_dim)
        q_out[:, pl.ds(pl.multiple_of(y_idx * q_cols + h * head_dim, head_dim), head_dim)] = rotate(q_bf[own_span, cols])
    y_copy.wait_recv()
    for h in range(q_cols // head_dim):
        cols = pl.ds(h * head_dim, head_dim)
        q_out[:, pl.ds(pl.multiple_of((1 - y_idx) * q_cols + h * head_dim, head_dim), head_dim)] = rotate(q_peer[:, cols])

    for pair in gu_outs:
        for item in pair:
            item.wait()
    for item in [hid_copy, gain_copy, q_copy, kv_copy, y_copy] + remote + remote_gu:
        item.wait_send()
    for step in range(1, x_size):
        stat_copy(step).wait_send()


def project_call(mesh, hidden, gain, cos_a, sin_a, w_query, w_key, w_value, w_gate, w_up):
    y_size, x_size = mesh.shape["yax"], mesh.shape["xax"]
    rows, part = hidden.shape
    own_rows = cos_a.shape[0]
    q_cols = w_query.shape[1]
    head_dim = w_key.shape[1]
    ff_cols = w_gate.shape[1] // x_size
    half = rows // 2
    dma, vm, f32, bf16 = pltpu.SemaphoreType.DMA, pltpu.VMEM, jnp.float32, jnp.bfloat16
    any_spec = pl.BlockSpec(memory_space=pl.ANY)
    vmem_spec = pl.BlockSpec(memory_space=pltpu.VMEM)
    shape = jax.ShapeDtypeStruct
    return pl.pallas_call(
        functools.partial(project_kernel, y_size, x_size),
        out_shape=(shape((own_rows, y_size * q_cols), bf16), shape((own_rows, head_dim), bf16),
                   shape((own_rows, head_dim), bf16), shape((rows, 2 * ff_cols), f32),
                   shape((half, 2 * ff_cols), f32), shape((half, 2 * ff_cols), f32)),
        in_specs=[vmem_spec] * 4 + [any_spec] * 5,
        out_specs=(vmem_spec,) * 3 + (any_spec,) * 3,
        scratch_shapes=[
            vm((rows, part), bf16), vm((8, part), f32), vm((2, part, q_cols), bf16), vm((2, part, 2 * head_dim), bf16),
            vm((2, 2, part, 2 * ff_cols), bf16),
            vm((2, rows, part), bf16), vm((8, rows), f32), vm((x_size, 8, rows), f32),
            vm((2 * own_rows, q_cols), f32), vm((2 * own_rows, q_cols), f32),
            vm((own_rows, 2 * head_dim), f32), vm((own_rows, 2 * head_dim), f32),
            vm((2 * own_rows, q_cols), bf16), vm((own_rows, q_cols), bf16),
            vm((2, 2, half, 2 * ff_cols), f32),
            dma((4,)), dma((x_size,)), dma((x_size,)), dma((7,)), dma((7,)), dma((7,)), dma((4,)), dma((2,)), dma((4,))],
        compiler_params=pltpu.CompilerParams(collective_id=1, has_side_effects=True, vmem_limit_bytes=40 * 1024 * 1024),
        cost_estimate=pl.CostEstimate(flops=2 * rows * part * 2 * (q_cols + 4 * ff_cols), bytes_accessed=30_000_000,
                                      transcendentals=0),
        name="project",
    )(hidden, jnp.broadcast_to(gain[None, :], (8, part)), cos_a, sin_a, w_query, w_key, w_value, w_gate, w_up)


S_CHUNK = 2048
SLOTS = 4


def attend_kernel(len_ref, q_ref, kn_ref, vn_ref, k_hbm, v_hbm, o_ref, k_buf, v_buf, s_buf, sem):
    n_seq, heads, head_dim = q_ref.shape
    scale = head_dim ** -0.5

    def n_chunks(b):
        return (len_ref[b] + (S_CHUNK - 1)) // S_CHUNK

    def copies(b, c, slot):
        span = pl.ds(pl.multiple_of(c * S_CHUNK, S_CHUNK), S_CHUNK)
        return (pltpu.make_async_copy(k_hbm.at[b, span, :], k_buf.at[slot], sem.at[0, slot]),
                pltpu.make_async_copy(v_hbm.at[b, span, :], v_buf.at[slot], sem.at[1, slot]))

    def advance(b, c):
        last = c + 1 >= n_chunks(jnp.minimum(b, n_seq - 1))
        return jnp.where(last, b + 1, b), jnp.where(last, 0, c + 1)

    def fetch(b, c, slot):
        @pl.when(b < n_seq)
        def _():
            for item in copies(b, c, slot):
                item.start()

    total = lax.fori_loop(0, n_seq, lambda b, acc: acc + n_chunks(b), 0)
    ahead = (0, 0)
    for i in range(SLOTS - 1):
        fetch(ahead[0], ahead[1], i)
        ahead = advance(*ahead)

    def scores(b, c, slot):
        raw = lax.dot_general(q_ref[b], k_buf[slot], NT_DIMS, preferred_element_type=jnp.float32) * scale
        pos = lax.broadcasted_iota(jnp.int32, (1, S_CHUNK), 1) + c * S_CHUNK
        return jnp.where(pos < len_ref[b], raw, -1e30)

    def fold(b, c, slot, s_val, state):
        run_max, run_sum, acc = state
        first = c == 0
        fresh = jnp.sum(q_ref[b].astype(jnp.float32) * kn_ref[b].astype(jnp.float32), axis=1, keepdims=True) * scale
        run_max = jnp.where(first, jnp.broadcast_to(fresh, run_max.shape), run_max)
        lane = lax.broadcasted_iota(jnp.int32, run_sum.shape, 1)
        run_sum = jnp.where(first, jnp.where(lane == 0, 1.0, 0.0), run_sum)
        acc = jnp.where(first, jnp.broadcast_to(vn_ref[b].astype(jnp.float32), acc.shape), acc)
        new_max = jnp.maximum(run_max, jnp.max(s_val, axis=1, keepdims=True))
        alpha = jnp.exp(run_max - new_max)
        prob = jnp.exp(s_val - new_max[:, 0:1])
        lanes = prob[:, 0:128]
        for g in range(1, S_CHUNK // 128):
            lanes = lanes + prob[:, g * 128:(g + 1) * 128]
        run_sum = run_sum * alpha + lanes
        acc = acc * alpha + jnp.dot(prob.astype(jnp.bfloat16), v_buf[slot], preferred_element_type=jnp.float32)

        @pl.when(c + 1 >= n_chunks(b))
        def _():
            o_ref[b] = (acc / jnp.sum(run_sum, axis=1, keepdims=True)).astype(jnp.bfloat16)
        return new_max, run_sum, acc

    for item in copies(0, 0, 0):
        item.wait()
    s_buf[...] = scores(0, 0, 0)
    zero = jnp.zeros((heads, 128), jnp.float32)

    def step(i, carry):
        b_prev, c_prev, b_next, c_next, b_ahead, c_ahead, state = carry
        slot_prev = lax.rem(i - 1, SLOTS)
        slot = lax.rem(i, SLOTS)
        fetch(b_ahead, c_ahead, lax.rem(i + SLOTS - 2, SLOTS))
        for item in copies(b_next, c_next, slot):
            item.wait()
        s_prev = s_buf[...]
        s_new = scores(b_next, c_next, slot)
        state = fold(b_prev, c_prev, slot_prev, s_prev, state)
        s_buf[...] = s_new
        return (b_next, c_next, *advance(b_next, c_next), *advance(b_ahead, c_ahead), state)

    b_one, c_one = advance(0, 0)
    carry = lax.fori_loop(1, total, step, (0, 0, b_one, c_one, ahead[0], ahead[1], (zero, zero, zero)))
    fold(carry[0], carry[1], lax.rem(total - 1, SLOTS), s_buf[...], carry[6])


def attend_call(query, k_cache, v_cache, key_new, value_new, lengths):
    n_seq, heads, head_dim = query.shape
    any_spec = pl.BlockSpec(memory_space=pl.ANY)
    vmem_spec = pl.BlockSpec(memory_space=pltpu.VMEM)
    return pl.pallas_call(
        attend_kernel,
        out_shape=jax.ShapeDtypeStruct(query.shape, jnp.bfloat16),
        in_specs=[pl.BlockSpec(memory_space=pltpu.SMEM), vmem_spec, vmem_spec, vmem_spec, any_spec, any_spec],
        out_specs=vmem_spec,
        scratch_shapes=[pltpu.VMEM((SLOTS, S_CHUNK, head_dim), jnp.bfloat16),
                        pltpu.VMEM((SLOTS, S_CHUNK, head_dim), jnp.bfloat16),
                        pltpu.VMEM((heads, S_CHUNK), jnp.float32), pltpu.SemaphoreType.DMA((2, SLOTS))],
        compiler_params=pltpu.CompilerParams(vmem_limit_bytes=32 * 1024 * 1024),
        cost_estimate=pl.CostEstimate(flops=40_000_000_000, bytes_accessed=130_000_000, transcendentals=4_000_000),
        name="attend",
    )(lengths, query, key_new[:, None, :], value_new[:, None, :], k_cache, v_cache)


def head_kernel(y_size, x_size, att_ref, hid_ref, gain_ref, keep_ref, got_a_ref, send_b_ref, w_out_ref, w_down_ref,
                emb_ref, z_ref, norm_ref, ebuf, f_own, f_peer, send, recv, o_all, m_all, w_out, w_down, gu_keep, gu_got,
                sum_own, sum_peer, mom_own, mom_all, stat_own, stat_all,
                own_sem, peer_ssem, peer_rsem, f_ssem, f_rsem, z_ssem, z_rsem, stat_ssem, stat_rsem, out_sem,
                o_ssem, o_rsem, m_ssem, m_rsem, in_sem, gu_sem, sum_ssem, sum_rsem, mom_ssem, mom_rsem):
    y_idx, d_idx, core, chip = positions(x_size)
    partner = 2 * chip + (1 - core)
    x_nbr = 2 * (1 - chip) + core
    x_diag = 2 * (1 - chip) + (1 - core)
    n_dev = y_size * x_size
    flat = y_idx * x_size + d_idx
    v_quarter = recv.shape[1]
    half = recv.shape[2]
    chunks = recv.shape[0]
    full_tiles = v_quarter // V_TILE
    tail = v_quarter - full_tiles * V_TILE
    own_rows = att_ref.shape[0]
    o_cols = o_all.shape[1]
    ff_cols = m_all.shape[3]
    part = hid_ref.shape[1]

    def e_own_copy(quarter, tile, size):
        place = x_nbr if quarter == 0 else d_idx
        start = pl.multiple_of(place * v_quarter + tile * V_TILE, 16)
        off = pl.multiple_of(tile * V_TILE, V_TILE)
        return pltpu.make_async_copy(emb_ref.at[pl.ds(start, size), :], ebuf.at[0, quarter, pl.ds(off, size), :],
                                     own_sem.at[quarter, tile])

    def e_peer_copy(quarter, tile, size):
        place = x_diag if quarter == 0 else partner
        start = pl.multiple_of(place * v_quarter + tile * V_TILE, 16)
        off = pl.multiple_of(tile * V_TILE, V_TILE)
        return pltpu.make_async_remote_copy(
            src_ref=emb_ref.at[pl.ds(start, size), :], dst_ref=ebuf.at[1, quarter, pl.ds(off, size), :],
            send_sem=peer_ssem.at[quarter, tile], recv_sem=peer_rsem.at[quarter, tile],
            device_id={"xax": partner}, device_id_type=MESH)

    def z_copy(chunk, tile, size):
        off = pl.multiple_of(tile * V_TILE, V_TILE)
        return pltpu.make_async_remote_copy(
            src_ref=send.at[chunk, pl.ds(off, size), :], dst_ref=recv.at[chunk, pl.ds(off, size), :],
            send_sem=z_ssem.at[chunk, tile], recv_sem=z_rsem.at[chunk, tile],
            device_id={"xax": x_nbr}, device_id_type=MESH)

    def to_xax(src, dst, ssem, rsem, place):
        return pltpu.make_async_remote_copy(src_ref=src, dst_ref=dst, send_sem=ssem, recv_sem=rsem,
                                            device_id={"xax": place}, device_id_type=MESH)

    def f_copy(chunk):
        return to_xax(f_own.at[chunk], f_peer.at[chunk], f_ssem.at[chunk], f_rsem.at[chunk], partner)

    def m_copy(chunk, which):
        slot, place = ((d_idx, partner), (d_idx, x_nbr), (x_nbr, partner))[which]
        return to_xax(m_all.at[chunk, slot], m_all.at[chunk, slot], m_ssem.at[chunk, which], m_rsem.at[chunk, which],
                      place)

    def sum_copy(chunk):
        return pltpu.make_async_remote_copy(
            src_ref=sum_own.at[chunk], dst_ref=sum_peer.at[chunk], send_sem=sum_ssem.at[chunk],
            recv_sem=sum_rsem.at[chunk], device_id={"yax": 1 - y_idx}, device_id_type=MESH)

    def mom_copy(chunk, step):
        return to_xax(mom_own.at[chunk], mom_all.at[chunk, d_idx], mom_ssem.at[chunk, step], mom_rsem.at[chunk, step],
                      lax.rem(d_idx + step, x_size))

    def o_copy(step):
        other = lax.rem(flat + step, n_dev)
        y_to = other // x_size
        return pltpu.make_async_remote_copy(
            src_ref=att_ref.at[:, pl.ds(pl.multiple_of(y_to * o_cols, 128), o_cols)],
            dst_ref=o_all.at[pl.ds(pl.multiple_of(flat * own_rows, own_rows), own_rows), :],
            send_sem=o_ssem.at[step], recv_sem=o_rsem.at[step],
            device_id={"yax": y_to, "xax": lax.rem(other, x_size)}, device_id_type=MESH)

    def over_tiles(body, low=0, high=None):
        high = full_tiles + 1 if high is None else high

        @pl.loop(low, min(high, full_tiles))
        def _(tile):
            body(tile, V_TILE)
        if high > full_tiles:
            body(full_tiles, tail)

    gu_copy = to_xax(send_b_ref, gu_got.at[1], gu_sem.at[0], gu_sem.at[1], x_nbr)
    ins = [pltpu.make_async_copy(keep_ref.at[pl.ds(0, half), :], gu_keep.at[0], in_sem.at[0]),
           pltpu.make_async_copy(got_a_ref, gu_got.at[0], in_sem.at[1]),
           pltpu.make_async_copy(w_out_ref, w_out, in_sem.at[2]),
           pltpu.make_async_copy(w_down_ref, w_down, in_sem.at[3]),
           pltpu.make_async_copy(keep_ref.at[pl.ds(half, half), :], gu_keep.at[1], in_sem.at[4])]
    for item in ins:
        item.start()
    all_barrier(y_size, x_size, y_idx, d_idx)

    def front_m(chunk):
        gated = gu_keep[chunk] + gu_got[chunk]
        gate = gated[:, :ff_cols].astype(jnp.bfloat16).astype(jnp.float32)
        up_val = gated[:, ff_cols:].astype(jnp.bfloat16).astype(jnp.float32)
        m_all[chunk, d_idx] = (gate * (1.0 / (1.0 + jnp.exp(-gate))) * up_val).astype(jnp.bfloat16)
        m_copy(chunk, 1).start()
        m_copy(chunk, 0).start()

    def front_rest(chunk):
        span = pl.ds(chunk * half, half)

        def down(slot):
            return jnp.dot(m_all[chunk, slot], w_down[pl.ds(pl.multiple_of(slot * ff_cols, ff_cols), ff_cols), :],
                           preferred_element_type=jnp.float32)
        sum_own[chunk] = jnp.dot(o_all[span, :], w_out[...], preferred_element_type=jnp.float32) + down(d_idx)
        m_copy(chunk, 0).wait_recv()
        sum_own[chunk] += down(partner)
        m_copy(chunk, 1).wait_recv()
        m_copy(chunk, 2).start()
        sum_own[chunk] += down(x_nbr)
        m_copy(chunk, 2).wait_recv()
        sum_own[chunk] += down(x_diag)
        sum_copy(chunk).start()
        sum_copy(chunk).wait_recv()
        res = hid_ref[span, :].astype(jnp.float32) + (sum_own[chunk] + sum_peer[chunk])
        packed = compact_rows(*local_moments(res))
        mom_own[chunk] = packed
        mom_all[chunk, d_idx] = packed
        for step in range(1, x_size):
            mom_copy(chunk, step).start()
        for step in range(1, x_size):
            mom_copy(chunk, step).wait_recv()
        mean, rstd = spread_rows(*join_moments([mom_all[chunk, i] for i in range(x_size)], x_size, part))
        f_own[chunk] = ((res - mean) * rstd * gain_ref[0:1, :]).astype(jnp.bfloat16)
        f_copy(chunk).start()

    def partial(chunk, quarter, tile, size):
        off = pl.multiple_of(tile * V_TILE, V_TILE)
        return (lax.dot_general(ebuf[0, quarter, pl.ds(off, size), :], f_own[chunk], NT_DIMS,
                                preferred_element_type=jnp.float32)
                + lax.dot_general(ebuf[1, quarter, pl.ds(off, size), :], f_peer[chunk], NT_DIMS,
                                  preferred_element_type=jnp.float32))

    def send_tiles(chunk, low, high):
        def one(tile, size):
            if chunk == 0:
                e_own_copy(0, tile, size).wait()
                e_peer_copy(0, tile, size).wait_recv()
            off = pl.multiple_of(tile * V_TILE, V_TILE)
            send[chunk, pl.ds(off, size), :] = partial(chunk, 0, tile, size)

        @pl.loop(low, min(high, full_tiles))
        def _(tile):
            one(tile, V_TILE)

            @pl.when(tile > low)
            def _():
                z_copy(chunk, tile - 1, V_TILE).start()
        if high > full_tiles:
            one(full_tiles, tail)
            z_copy(chunk, full_tiles - 1, V_TILE).start()
            z_copy(chunk, full_tiles, tail).start()
        else:
            z_copy(chunk, high - 1, V_TILE).start()

    def out_copy(chunk, tile, size):
        span = pl.ds(pl.multiple_of(tile * V_TILE, V_TILE), size)
        return pltpu.make_async_copy(recv.at[chunk, span, :], z_ref.at[span, pl.ds(chunk * half, half)],
                                     out_sem.at[chunk, tile])

    def take_tile(chunk, tile, size, carry):
        run_max, run_sum = carry
        off = pl.multiple_of(tile * V_TILE, V_TILE)
        if chunk == 0:
            e_own_copy(1, tile, size).wait()
            e_peer_copy(1, tile, size).wait_recv()
        own = partial(chunk, 1, tile, size)
        z_copy(chunk, tile, size).wait_recv()
        z_val = own + recv[chunk, pl.ds(off, size), :]
        recv[chunk, pl.ds(off, size), :] = z_val
        z_grp = z_val.reshape(size // 8, 8, half)
        new_max = jnp.maximum(run_max, jnp.max(z_grp, axis=0))
        new_sum = run_sum * jnp.exp(run_max - new_max) + jnp.sum(jnp.exp(z_grp - new_max[None]), axis=0)
        out_copy(chunk, tile, size).start()
        return new_max, new_sum

    def stat_copy(chunk, step):
        other = lax.rem(flat + step, n_dev)
        return pltpu.make_async_remote_copy(
            src_ref=stat_own.at[chunk], dst_ref=stat_all.at[chunk, flat], send_sem=stat_ssem.at[chunk, step],
            recv_sem=stat_rsem.at[chunk, step],
            device_id={"yax": other // x_size, "xax": lax.rem(other, x_size)}, device_id_type=MESH)

    def gather_chunk(chunk):
        low = jnp.full((8, half), -jnp.inf, jnp.float32)
        carry = take_tile(chunk, 0, V_TILE, (low, jnp.zeros((8, half), jnp.float32)))
        carry = lax.fori_loop(1, full_tiles, lambda tile, c: take_tile(chunk, tile, V_TILE, c), carry)
        run_max, run_sum = take_tile(chunk, full_tiles, tail, carry)
        top = jnp.max(run_max, axis=0, keepdims=True)
        total = jnp.sum(run_sum * jnp.exp(run_max - top), axis=0, keepdims=True)
        sub = lax.broadcasted_iota(jnp.int32, (8, half), 0)
        both = jnp.where(sub == 0, top, total)
        stat_own[chunk] = both
        stat_all[chunk, flat] = both
        for step in range(1, n_dev):
            stat_copy(chunk, step).start()

    def norm_chunk(chunk):
        for step in range(1, n_dev):
            stat_copy(chunk, step).wait_recv()
        tops = [stat_all[chunk, i, 0:1, :] for i in range(n_dev)]
        top_all = tops[0]
        for item in tops[1:]:
            top_all = jnp.maximum(top_all, item)
        sum_all = jnp.zeros_like(top_all)
        for i in range(n_dev):
            sum_all = sum_all + stat_all[chunk, i, 1:2, :] * jnp.exp(tops[i] - top_all)
        norm_ref[:, pl.ds(chunk * half, half)] = top_all + jnp.log(sum_all)

    ins[0].wait()
    ins[1].wait()
    front_m(0)
    for step in range(1, n_dev):
        o_copy(step).start()
    gu_copy.start()
    over_tiles(lambda tile, size: e_own_copy(0, tile, size).start())
    over_tiles(lambda tile, size: e_peer_copy(0, tile, size).start())
    over_tiles(lambda tile, size: e_own_copy(1, tile, size).start())
    over_tiles(lambda tile, size: e_peer_copy(1, tile, size).start())
    o_all[pl.ds(pl.multiple_of(flat * own_rows, own_rows), own_rows), :] = att_ref[
        :, pl.ds(pl.multiple_of(y_idx * o_cols, 128), o_cols)]
    ins[2].wait()
    ins[3].wait()
    for step in range(1, n_dev):
        o_copy(step).wait_recv()
    front_rest(0)
    f_copy(0).wait_recv()
    split = full_tiles // 2
    send_tiles(0, 0, split)
    ins[4].wait()
    gu_copy.wait_recv()
    front_m(1)
    send_tiles(0, split, full_tiles + 1)
    front_rest(1)
    f_copy(1).wait_recv()
    send_tiles(1, 0, full_tiles + 1)
    for chunk in range(chunks):
        gather_chunk(chunk)
    for chunk in range(chunks):
        norm_chunk(chunk)

    gu_copy.wait_send()
    for step in range(1, n_dev):
        o_copy(step).wait_send()
    for chunk in range(chunks):
        f_copy(chunk).wait_send()
        sum_copy(chunk).wait_send()
        for which in range(3):
            m_copy(chunk, which).wait_send()
        for step in range(1, x_size):
            mom_copy(chunk, step).wait_send()
        for step in range(1, n_dev):
            stat_copy(chunk, step).wait_send()
        over_tiles(lambda tile, size: z_copy(chunk, tile, size).wait_send())
        over_tiles(lambda tile, size: e_peer_copy(chunk, tile, size).wait_send())
        over_tiles(lambda tile, size: out_copy(chunk, tile, size).wait())


def head_call(mesh, attn_own, hidden, gain, keep, got_a, send_b, w_out, w_down, embedding):
    y_size, x_size = mesh.shape["yax"], mesh.shape["xax"]
    rows, part = hidden.shape
    v_quarter = embedding.shape[0] // x_size
    half = rows // 2
    tiles = v_quarter // V_TILE + 1
    n_dev = y_size * x_size
    o_cols = w_out.shape[0]
    ff_cols = w_down.shape[0] // x_size
    dma, vm, f32, bf16 = pltpu.SemaphoreType.DMA, pltpu.VMEM, jnp.float32, jnp.bfloat16
    any_spec = pl.BlockSpec(memory_space=pl.ANY)
    vmem_spec = pl.BlockSpec(memory_space=pltpu.VMEM)
    return pl.pallas_call(
        functools.partial(head_kernel, y_size, x_size),
        out_shape=(jax.ShapeDtypeStruct((v_quarter, rows), f32), jax.ShapeDtypeStruct((1, rows), f32)),
        in_specs=[vmem_spec] * 3 + [any_spec] * 6,
        out_specs=(any_spec, vmem_spec),
        scratch_shapes=[
            vm((2, 2, v_quarter, part), bf16), vm((2, half, part), bf16), vm((2, half, part), bf16),
            vm((2, v_quarter, half), f32), vm((2, v_quarter, half), f32),
            vm((rows, o_cols), bf16), vm((2, x_size, half, ff_cols), bf16), vm(w_out.shape, bf16), vm(w_down.shape, bf16),
            vm((2, half, 2 * ff_cols), f32), vm((2, half, 2 * ff_cols), f32),
            vm((2, half, part), f32), vm((2, half, part), f32),
            vm((2, 8, half), f32), vm((2, x_size, 8, half), f32), vm((2, 8, half), f32), vm((2, n_dev, 8, half), f32),
            dma((2, tiles)), dma((2, tiles)), dma((2, tiles)), dma((2,)), dma((2,)), dma((2, tiles)), dma((2, tiles)),
            dma((2, n_dev)), dma((2, n_dev)), dma((2, tiles)),
            dma((n_dev,)), dma((n_dev,)), dma((2, 3)), dma((2, 3)), dma((5,)), dma((2,)), dma((2,)), dma((2,)),
            dma((2, x_size)), dma((2, x_size))],
        compiler_params=pltpu.CompilerParams(collective_id=0, has_side_effects=True,
                                             vmem_limit_bytes=63 * 1024 * 1024),
        cost_estimate=pl.CostEstimate(flops=2 * rows * 2 * v_quarter * 2 * part, bytes_accessed=40_000_000,
                                      transcendentals=rows * v_quarter),
        name="head",
    )(attn_own, hidden, jnp.broadcast_to(gain[None, :], (8, part)), keep, got_a, send_b, w_out, w_down, embedding)


def solution(mesh):
    y_size = mesh.shape["yax"]
    x_size = mesh.shape["xax"]
    row_spec = P(("dp", "yax", "xax"))

    def local_step(hidden, cache_len, k_cache, v_cache, g_attn, w_query, w_key, w_value,
                   w_gate, w_up, w_out, w_down, g_final, embedding):
        rows = hidden.shape[0]
        own_rows = k_cache.shape[0]
        head_dim = k_cache.shape[2]
        heads = y_size * w_query.shape[1] // head_dim
        own_start = (lax.axis_index("yax") * x_size + lax.axis_index("xax")) * own_rows
        len_own = lax.dynamic_slice_in_dim(cache_len, own_start, own_rows, axis=0)
        angles = rope_angle(len_own, head_dim)
        cos_a, sin_a = jnp.cos(angles), jnp.sin(angles)
        cos_a = jnp.concatenate([cos_a, cos_a], axis=1)
        sin_a = jnp.concatenate([-sin_a, sin_a], axis=1)
        query, key_own, value_own, keep, send_a, send_b = project_call(
            mesh, hidden, g_attn, cos_a, sin_a, w_query, w_key, w_value, w_gate, w_up)
        got_a = lax.ppermute(send_a, "xax", [(i, (i + x_size // 2) % x_size) for i in range(x_size)])
        attn_own = attend_call(query.reshape(own_rows, heads, head_dim), k_cache, v_cache, key_own, value_own, len_own)
        z_val, log_norm = head_call(mesh, attn_own.reshape(own_rows, heads * head_dim), hidden, g_final, keep, got_a,
                                    send_b, w_out, w_down, embedding)
        return key_own, value_own, (z_val - log_norm).T, log_norm.reshape(rows)

    in_specs = (P("dp", "xax"), P("dp"), row_spec, row_spec, P("xax"), P("xax", "yax"),
                P("xax", None), P("xax", None), P("xax", "yax"), P("xax", "yax"),
                P("yax", "xax"), P("yax", "xax"), P("xax"), P("yax", "xax"))
    out_specs = (row_spec, row_spec, P("dp", ("yax", "xax")), P("dp"))
    return jax.shard_map(local_step, mesh=mesh, in_specs=in_specs, out_specs=out_specs, check_vma=False)
```

```python
import functools

import jax
import jax.numpy as jnp
from jax import lax
from jax.experimental import pallas as pl
from jax.experimental.pallas import tpu as pltpu
from jax.sharding import PartitionSpec as P

EPS = 1e-6
ROPE_BASE = 10000.0


def rope_angle(positions, head_dim):
    half_dim = head_dim // 2
    inv_freq = ROPE_BASE ** (-(jnp.arange(half_dim, dtype=jnp.float32) * 2.0) / head_dim)
    return positions.astype(jnp.float32)[:, None] * inv_freq[None, :]


MESH = pl.DeviceIdType.MESH
V_TILE = 512
NT_DIMS = (((1,), (1,)), ((), ()))


def positions(x_size):
    y_idx = lax.axis_index("yax")
    d_idx = lax.axis_index("xax")
    core = lax.rem(d_idx, 2)
    chip = d_idx // 2
    return y_idx, d_idx, core, chip


def all_barrier(y_size, x_size, y_idx, d_idx):
    barrier = pltpu.get_barrier_semaphore()
    for step in range(1, y_size * x_size):
        flat = lax.rem(y_idx * x_size + d_idx + step, y_size * x_size)
        pl.semaphore_signal(barrier, inc=1, device_id={"yax": flat // x_size, "xax": lax.rem(flat, x_size)},
                            device_id_type=MESH)
    pl.semaphore_wait(barrier, y_size * x_size - 1)


def compact_rows(first, second):
    rows = first.shape[0]
    lane = lax.broadcasted_iota(jnp.int32, (rows, 128), 1)
    return jnp.transpose(jnp.where(lane == 0, first, second))[0:8, :]


def spread_rows(first, second):
    rows = first.shape[1]
    sub = lax.broadcasted_iota(jnp.int32, (128, rows), 0)
    cols = jnp.transpose(jnp.where(sub == 0, first, second))
    return cols[:, 0:1], cols[:, 1:2]


def local_moments(values_in):
    part = values_in.shape[1]
    mean = jnp.sum(values_in, axis=1, keepdims=True) / part
    diff = values_in - mean
    return mean, jnp.sum(diff * diff, axis=1, keepdims=True)


def join_moments(stats, count, part):
    mean = stats[0][0:1, :]
    for item in stats[1:]:
        mean = mean + item[0:1, :]
    mean = mean / count
    square = jnp.zeros_like(mean)
    for item in stats:
        shift = item[0:1, :] - mean
        square = square + item[1:2, :] + part * shift * shift
    return mean, lax.rsqrt(square / (count * part) + EPS)


def project_kernel(y_size, x_size, hid_ref, gain_ref, cos_ref, sin_ref, wq_ref, wk_ref, wv_ref, wg_ref, wu_ref,
                   q_out, k_out, v_out, keep_out, send_a_out, send_b_out,
                   hid_peer, gain_own, gain_peer, wq_buf, wkv_buf, wgu_buf, n_buf, stat_own, stat_all,
                   q_send, q_recv, kv_send, kv_recv, q_bf, q_peer, gu_buf,
                   hid_sem, stat_ssem, stat_rsem, wl_sem, wp_ssem, wp_rsem, q_sem, y_sem, out_sem):
    y_idx, d_idx, core, chip = positions(x_size)
    partner = 2 * chip + (1 - core)
    x_nbr = 2 * (1 - chip) + core
    rows, part = hid_ref.shape
    half = rows // 2
    own_rows = q_out.shape[0]
    q_cols = wq_ref.shape[1]
    head_dim = wk_ref.shape[1]
    ff_cols = wgu_buf.shape[3] // 2
    n_blk = rows // own_rows

    def ff_block(j, which_core):
        place = (2 * (1 - chip) if j == 0 else 2 * chip) + which_core
        return pl.ds(pl.multiple_of(place * ff_cols, 128), ff_cols)

    def small_dsts(side):
        return (wq_buf.at[side], wkv_buf.at[side, :, pl.ds(0, head_dim)], wkv_buf.at[side, :, pl.ds(head_dim, head_dim)])

    local = [pltpu.make_async_copy(src, dst, wl_sem.at[i])
             for i, (src, dst) in enumerate(zip((wq_ref, wk_ref, wv_ref), small_dsts(0)))]
    remote = [pltpu.make_async_remote_copy(src_ref=src, dst_ref=dst, send_sem=wp_ssem.at[i], recv_sem=wp_rsem.at[i],
                                           device_id={"xax": partner}, device_id_type=MESH)
              for i, (src, dst) in enumerate(zip((wq_ref, wk_ref, wv_ref), small_dsts(1)))]
    local_gu, remote_gu = [], []
    for j in range(2):
        for which, src in enumerate((wg_ref, wu_ref)):
            i = 3 + 2 * j + which
            dst_cols = pl.ds(which * ff_cols, ff_cols)
            local_gu.append(pltpu.make_async_copy(src.at[:, ff_block(j, core)], wgu_buf.at[0, j, :, dst_cols],
                                                  wl_sem.at[i]))
            remote_gu.append(pltpu.make_async_remote_copy(
                src_ref=src.at[:, ff_block(j, 1 - core)], dst_ref=wgu_buf.at[1, j, :, dst_cols],
                send_sem=wp_ssem.at[i], recv_sem=wp_rsem.at[i], device_id={"xax": partner}, device_id_type=MESH))
    hid_copy = pltpu.make_async_remote_copy(src_ref=hid_ref, dst_ref=hid_peer, send_sem=hid_sem.at[0],
                                            recv_sem=hid_sem.at[1], device_id={"xax": partner}, device_id_type=MESH)
    gain_copy = pltpu.make_async_remote_copy(src_ref=gain_own, dst_ref=gain_peer, send_sem=hid_sem.at[2],
                                             recv_sem=hid_sem.at[3], device_id={"xax": partner}, device_id_type=MESH)

    def stat_copy(step):
        return pltpu.make_async_remote_copy(
            src_ref=stat_own, dst_ref=stat_all.at[d_idx], send_sem=stat_ssem.at[step], recv_sem=stat_rsem.at[step],
            device_id={"xax": lax.rem(d_idx + step, x_size)}, device_id_type=MESH)

    for item in local:
        item.start()
    gain_own[...] = jnp.broadcast_to(gain_ref[...], gain_own.shape)
    all_barrier(y_size, x_size, y_idx, d_idx)
    hid_copy.start()
    gain_copy.start()
    for item in remote:
        item.start()
    for item in local_gu:
        item.start()

    hid = hid_ref[...].astype(jnp.float32)
    mean_own, square_own = local_moments(hid)
    packed = compact_rows(mean_own, square_own)
    stat_own[...] = packed
    stat_all[d_idx] = packed
    for step in range(1, x_size):
        stat_copy(step).start()
    for item in remote_gu:
        item.start()
    hid_copy.wait_recv()
    gain_copy.wait_recv()
    for step in range(1, x_size):
        stat_copy(step).wait_recv()
    mean, rstd = spread_rows(*join_moments([stat_all[i] for i in range(x_size)], x_size, part))
    n_buf[0] = ((hid - mean) * rstd * gain_ref[0:1, :]).astype(jnp.bfloat16)
    n_buf[1] = ((hid_peer[...].astype(jnp.float32) - mean) * rstd * gain_peer[0:1, :]).astype(jnp.bfloat16)

    def dest_rows(y_at, chip_at):
        return pl.ds(pl.multiple_of(y_at * half + (2 * chip_at + core) * own_rows, own_rows), own_rows)

    def two_dots(row_sets, weights):
        left = [jnp.concatenate([n_buf[side, r, :] for r in row_sets], axis=0) if len(row_sets) > 1
                else n_buf[side, row_sets[0], :] for side in range(2)]
        return (jnp.dot(left[0], weights.at[0][...], preferred_element_type=jnp.float32)
                + jnp.dot(left[1], weights.at[1][...], preferred_element_type=jnp.float32))

    for item in local:
        item.wait()
    for item in remote:
        item.wait_recv()
    q_send[...] = two_dots([dest_rows(0, 1 - chip), dest_rows(1, 1 - chip)], wq_buf)
    kv_send[...] = two_dots([dest_rows(y_idx, 1 - chip)], wkv_buf)
    q_copy = pltpu.make_async_remote_copy(src_ref=q_send, dst_ref=q_recv, send_sem=q_sem.at[0], recv_sem=q_sem.at[1],
                                          device_id={"xax": x_nbr}, device_id_type=MESH)
    kv_copy = pltpu.make_async_remote_copy(src_ref=kv_send, dst_ref=kv_recv, send_sem=q_sem.at[2],
                                           recv_sem=q_sem.at[3], device_id={"xax": x_nbr}, device_id_type=MESH)
    q_copy.start()
    q_keep = two_dots([dest_rows(0, chip), dest_rows(1, chip)], wq_buf)
    kv_copy.start()
    kv_keep = two_dots([dest_rows(y_idx, chip)], wkv_buf)

    for item in local_gu:
        item.wait()
    for item in remote_gu:
        item.wait_recv()

    gu_outs = [[pltpu.make_async_copy(gu_buf.at[0, 0], send_a_out, out_sem.at[0]),
                pltpu.make_async_copy(gu_buf.at[0, 1], send_b_out, out_sem.at[1])],
               [pltpu.make_async_copy(gu_buf.at[1, r], keep_out.at[pl.ds(r * half, half), :], out_sem.at[2 + r])
                for r in range(2)]]

    def gu_part(j, r):
        span = pl.ds(r * half, half)

        @pl.loop(0, 2 * ff_cols // 512)
        def _(t):
            cols = pl.ds(pl.multiple_of(t * 512, 512), 512)
            gu_buf[j, r, :, cols] = (
                jnp.dot(n_buf[0, span, :], wgu_buf[0, j, :, cols], preferred_element_type=jnp.float32)
                + jnp.dot(n_buf[1, span, :], wgu_buf[1, j, :, cols], preferred_element_type=jnp.float32))

    for r in range(2):
        gu_part(0, r)
        gu_outs[0][r].start()

    def rotate(values_in):
        val = values_in.astype(jnp.float32)
        return (val * cos_ref[...] + pltpu.roll(val, head_dim // 2, 1) * sin_ref[...]).astype(jnp.bfloat16)

    q_copy.wait_recv()
    q_bf[...] = (q_keep + q_recv[...]).astype(jnp.bfloat16)
    y_copy = pltpu.make_async_remote_copy(
        src_ref=q_bf.at[pl.ds(pl.multiple_of((1 - y_idx) * own_rows, own_rows), own_rows), :], dst_ref=q_peer,
        send_sem=y_sem.at[0], recv_sem=y_sem.at[1], device_id={"yax": 1 - y_idx}, device_id_type=MESH)
    y_copy.start()
    kv_copy.wait_recv()
    kv_bf = (kv_keep + kv_recv[...]).astype(jnp.bfloat16)
    k_out[...] = rotate(kv_bf[:, :head_dim])
    v_out[...] = kv_bf[:, head_dim:]
    for r in range(2):
        gu_part(1, r)
        gu_outs[1][r].start()
    own_span = pl.ds(pl.multiple_of(y_idx * own_rows, own_rows), own_rows)
    for h in range(q_cols // head_dim):
        cols = pl.ds(h * head_dim, head_dim)
        q_out[:, pl.ds(pl.multiple_of(y_idx * q_cols + h * head_dim, head_dim), head_dim)] = rotate(q_bf[own_span, cols])
    y_copy.wait_recv()
    for h in range(q_cols // head_dim):
        cols = pl.ds(h * head_dim, head_dim)
        q_out[:, pl.ds(pl.multiple_of((1 - y_idx) * q_cols + h * head_dim, head_dim), head_dim)] = rotate(q_peer[:, cols])

    for pair in gu_outs:
        for item in pair:
            item.wait()
    for item in [hid_copy, gain_copy, q_copy, kv_copy, y_copy] + remote + remote_gu:
        item.wait_send()
    for step in range(1, x_size):
        stat_copy(step).wait_send()


def project_call(mesh, hidden, gain, cos_a, sin_a, w_query, w_key, w_value, w_gate, w_up):
    y_size, x_size = mesh.shape["yax"], mesh.shape["xax"]
    rows, part = hidden.shape
    own_rows = cos_a.shape[0]
    q_cols = w_query.shape[1]
    head_dim = w_key.shape[1]
    ff_cols = w_gate.shape[1] // x_size
    half = rows // 2
    dma, vm, f32, bf16 = pltpu.SemaphoreType.DMA, pltpu.VMEM, jnp.float32, jnp.bfloat16
    any_spec = pl.BlockSpec(memory_space=pl.ANY)
    vmem_spec = pl.BlockSpec(memory_space=pltpu.VMEM)
    shape = jax.ShapeDtypeStruct
    return pl.pallas_call(
        functools.partial(project_kernel, y_size, x_size),
        out_shape=(shape((own_rows, y_size * q_cols), bf16), shape((own_rows, head_dim), bf16),
                   shape((own_rows, head_dim), bf16), shape((rows, 2 * ff_cols), f32),
                   shape((half, 2 * ff_cols), f32), shape((half, 2 * ff_cols), f32)),
        in_specs=[vmem_spec] * 4 + [any_spec] * 5,
        out_specs=(vmem_spec,) * 3 + (any_spec,) * 3,
        scratch_shapes=[
            vm((rows, part), bf16), vm((8, part), f32), vm((8, part), f32), vm((2, part, q_cols), bf16), vm((2, part, 2 * head_dim), bf16),
            vm((2, 2, part, 2 * ff_cols), bf16),
            vm((2, rows, part), bf16), vm((8, rows), f32), vm((x_size, 8, rows), f32),
            vm((2 * own_rows, q_cols), f32), vm((2 * own_rows, q_cols), f32),
            vm((own_rows, 2 * head_dim), f32), vm((own_rows, 2 * head_dim), f32),
            vm((2 * own_rows, q_cols), bf16), vm((own_rows, q_cols), bf16),
            vm((2, 2, half, 2 * ff_cols), f32),
            dma((4,)), dma((x_size,)), dma((x_size,)), dma((7,)), dma((7,)), dma((7,)), dma((4,)), dma((2,)), dma((4,))],
        compiler_params=pltpu.CompilerParams(collective_id=1, has_side_effects=True, vmem_limit_bytes=63 * 1024 * 1024),
        cost_estimate=pl.CostEstimate(flops=2 * rows * part * 2 * (q_cols + 4 * ff_cols), bytes_accessed=30_000_000,
                                      transcendentals=0),
        name="project",
    )(hidden, gain[None, :], cos_a, sin_a, w_query, w_key, w_value, w_gate, w_up)


S_CHUNK = 2048
SLOTS = 4


def attend_kernel(len_ref, q_ref, kn_ref, vn_ref, k_hbm, v_hbm, o_ref, k_out, v_out, kn_buf, vn_buf, k_buf, v_buf, s_buf,
                  sem):
    n_seq, heads, head_dim = q_ref.shape
    scale = head_dim ** -0.5

    def n_chunks(b):
        return (len_ref[b] + (S_CHUNK - 1)) // S_CHUNK

    def copies(b, c, slot):
        span = pl.ds(pl.multiple_of(c * S_CHUNK, S_CHUNK), S_CHUNK)
        return (pltpu.make_async_copy(k_hbm.at[b, span, :], k_buf.at[slot], sem.at[0, slot]),
                pltpu.make_async_copy(v_hbm.at[b, span, :], v_buf.at[slot], sem.at[1, slot]))

    def advance(b, c):
        last = c + 1 >= n_chunks(jnp.minimum(b, n_seq - 1))
        return jnp.where(last, b + 1, b), jnp.where(last, 0, c + 1)

    def fetch(b, c, slot):
        @pl.when(b < n_seq)
        def _():
            for item in copies(b, c, slot):
                item.start()

    total = lax.fori_loop(0, n_seq, lambda b, acc: acc + n_chunks(b), 0)
    ahead = (0, 0)
    for i in range(SLOTS - 1):
        fetch(ahead[0], ahead[1], i)
        ahead = advance(*ahead)

    k_out[...] = kn_ref[...]
    v_out[...] = vn_ref[...]
    kn_buf[...] = kn_ref[...].astype(jnp.float32)
    vn_buf[...] = vn_ref[...].astype(jnp.float32)

    def scores(b, c, slot):
        raw = lax.dot_general(q_ref[b], k_buf[slot], NT_DIMS, preferred_element_type=jnp.float32) * scale
        pos = lax.broadcasted_iota(jnp.int32, (1, S_CHUNK), 1) + c * S_CHUNK
        return jnp.where(pos < len_ref[b], raw, -1e30)

    def fold(b, c, slot, s_val, state):
        run_max, run_sum, acc = state
        first = c == 0
        fresh = jnp.sum(q_ref[b].astype(jnp.float32) * kn_buf[pl.ds(b, 1), :], axis=1, keepdims=True) * scale
        run_max = jnp.where(first, jnp.broadcast_to(fresh, run_max.shape), run_max)
        lane = lax.broadcasted_iota(jnp.int32, run_sum.shape, 1)
        run_sum = jnp.where(first, jnp.where(lane == 0, 1.0, 0.0), run_sum)
        acc = jnp.where(first, jnp.broadcast_to(vn_buf[pl.ds(b, 1), :], acc.shape), acc)
        new_max = jnp.maximum(run_max, jnp.max(s_val, axis=1, keepdims=True))
        alpha = jnp.exp(run_max - new_max)
        prob = jnp.exp(s_val - new_max[:, 0:1])
        lanes = prob[:, 0:128]
        for g in range(1, S_CHUNK // 128):
            lanes = lanes + prob[:, g * 128:(g + 1) * 128]
        run_sum = run_sum * alpha + lanes
        acc = acc * alpha + jnp.dot(prob.astype(jnp.bfloat16), v_buf[slot], preferred_element_type=jnp.float32)

        @pl.when(c + 1 >= n_chunks(b))
        def _():
            o_ref[b] = (acc / jnp.sum(run_sum, axis=1, keepdims=True)).astype(jnp.bfloat16)
        return new_max, run_sum, acc

    for item in copies(0, 0, 0):
        item.wait()
    s_buf[...] = scores(0, 0, 0)
    zero = jnp.zeros((heads, 128), jnp.float32)

    def step(i, carry):
        b_prev, c_prev, b_next, c_next, b_ahead, c_ahead, state = carry
        slot_prev = lax.rem(i - 1, SLOTS)
        slot = lax.rem(i, SLOTS)
        fetch(b_ahead, c_ahead, lax.rem(i + SLOTS - 2, SLOTS))
        for item in copies(b_next, c_next, slot):
            item.wait()
        s_prev = s_buf[...]
        s_new = scores(b_next, c_next, slot)
        state = fold(b_prev, c_prev, slot_prev, s_prev, state)
        s_buf[...] = s_new
        return (b_next, c_next, *advance(b_next, c_next), *advance(b_ahead, c_ahead), state)

    b_one, c_one = advance(0, 0)
    carry = lax.fori_loop(1, total, step, (0, 0, b_one, c_one, ahead[0], ahead[1], (zero, zero, zero)))
    fold(carry[0], carry[1], lax.rem(total - 1, SLOTS), s_buf[...], carry[6])


def attend_call(query, k_cache, v_cache, key_new, value_new, lengths):
    n_seq, heads, head_dim = query.shape
    any_spec = pl.BlockSpec(memory_space=pl.ANY)
    vmem_spec = pl.BlockSpec(memory_space=pltpu.VMEM)
    return pl.pallas_call(
        attend_kernel,
        out_shape=(jax.ShapeDtypeStruct(query.shape, jnp.bfloat16), jax.ShapeDtypeStruct(key_new.shape, jnp.bfloat16),
                   jax.ShapeDtypeStruct(key_new.shape, jnp.bfloat16)),
        in_specs=[pl.BlockSpec(memory_space=pltpu.SMEM), vmem_spec, vmem_spec, vmem_spec, any_spec, any_spec],
        out_specs=(vmem_spec, vmem_spec, vmem_spec),
        scratch_shapes=[pltpu.VMEM(key_new.shape, jnp.float32), pltpu.VMEM(key_new.shape, jnp.float32),
                        pltpu.VMEM((SLOTS, S_CHUNK, head_dim), jnp.bfloat16),
                        pltpu.VMEM((SLOTS, S_CHUNK, head_dim), jnp.bfloat16),
                        pltpu.VMEM((heads, S_CHUNK), jnp.float32), pltpu.SemaphoreType.DMA((2, SLOTS))],
        compiler_params=pltpu.CompilerParams(vmem_limit_bytes=63 * 1024 * 1024),
        cost_estimate=pl.CostEstimate(flops=40_000_000_000, bytes_accessed=130_000_000, transcendentals=4_000_000),
        name="attend",
    )(lengths, query, key_new, value_new, k_cache, v_cache)


def head_kernel(y_size, x_size, att_ref, hid_ref, gain_ref, keep_ref, got_a_ref, got_b_ref, w_out_ref, w_down_ref,
                emb_ref, z_ref, norm_ref, ebuf, f_own, f_peer, send, recv, o_all, m_all, w_out, w_down, gu_keep, gu_got,
                sum_own, sum_peer, mom_own, mom_all, stat_own, stat_all,
                own_sem, peer_ssem, peer_rsem, f_ssem, f_rsem, z_ssem, z_rsem, stat_ssem, stat_rsem, out_sem,
                o_ssem, o_rsem, m_ssem, m_rsem, in_sem, sum_ssem, sum_rsem, mom_ssem, mom_rsem):
    y_idx, d_idx, core, chip = positions(x_size)
    partner = 2 * chip + (1 - core)
    x_nbr = 2 * (1 - chip) + core
    x_diag = 2 * (1 - chip) + (1 - core)
    n_dev = y_size * x_size
    flat = y_idx * x_size + d_idx
    v_quarter = recv.shape[1]
    half = recv.shape[2]
    chunks = recv.shape[0]
    full_tiles = v_quarter // V_TILE
    tail = v_quarter - full_tiles * V_TILE
    own_rows = att_ref.shape[0]
    o_cols = o_all.shape[1]
    ff_cols = m_all.shape[3]
    part = hid_ref.shape[1]

    def e_own_copy(quarter, tile, size):
        place = x_nbr if quarter == 0 else d_idx
        start = pl.multiple_of(place * v_quarter + tile * V_TILE, 16)
        off = pl.multiple_of(tile * V_TILE, V_TILE)
        return pltpu.make_async_copy(emb_ref.at[pl.ds(start, size), :], ebuf.at[0, quarter, pl.ds(off, size), :],
                                     own_sem.at[quarter, tile])

    def e_peer_copy(quarter, tile, size):
        place = x_diag if quarter == 0 else partner
        start = pl.multiple_of(place * v_quarter + tile * V_TILE, 16)
        off = pl.multiple_of(tile * V_TILE, V_TILE)
        return pltpu.make_async_remote_copy(
            src_ref=emb_ref.at[pl.ds(start, size), :], dst_ref=ebuf.at[1, quarter, pl.ds(off, size), :],
            send_sem=peer_ssem.at[quarter, tile], recv_sem=peer_rsem.at[quarter, tile],
            device_id={"xax": partner}, device_id_type=MESH)

    def z_copy(chunk, tile, size):
        off = pl.multiple_of(tile * V_TILE, V_TILE)
        return pltpu.make_async_remote_copy(
            src_ref=send.at[chunk, pl.ds(off, size), :], dst_ref=recv.at[chunk, pl.ds(off, size), :],
            send_sem=z_ssem.at[chunk, tile], recv_sem=z_rsem.at[chunk, tile],
            device_id={"xax": x_nbr}, device_id_type=MESH)

    def to_xax(src, dst, ssem, rsem, place):
        return pltpu.make_async_remote_copy(src_ref=src, dst_ref=dst, send_sem=ssem, recv_sem=rsem,
                                            device_id={"xax": place}, device_id_type=MESH)

    def f_copy(chunk):
        return to_xax(f_own.at[chunk], f_peer.at[chunk], f_ssem.at[chunk], f_rsem.at[chunk], partner)

    def m_copy(chunk, which):
        slot, place = ((d_idx, partner), (d_idx, x_nbr), (x_nbr, partner))[which]
        return to_xax(m_all.at[chunk, slot], m_all.at[chunk, slot], m_ssem.at[chunk, which], m_rsem.at[chunk, which],
                      place)

    def sum_copy(chunk):
        return pltpu.make_async_remote_copy(
            src_ref=sum_own.at[chunk], dst_ref=sum_peer.at[chunk], send_sem=sum_ssem.at[chunk],
            recv_sem=sum_rsem.at[chunk], device_id={"yax": 1 - y_idx}, device_id_type=MESH)

    def mom_copy(chunk, step):
        return to_xax(mom_own.at[chunk], mom_all.at[chunk, d_idx], mom_ssem.at[chunk, step], mom_rsem.at[chunk, step],
                      lax.rem(d_idx + step, x_size))

    def o_copy(step):
        other = lax.rem(flat + step, n_dev)
        y_to = other // x_size
        return pltpu.make_async_remote_copy(
            src_ref=att_ref.at[:, pl.ds(pl.multiple_of(y_to * o_cols, 128), o_cols)],
            dst_ref=o_all.at[pl.ds(pl.multiple_of(flat * own_rows, own_rows), own_rows), :],
            send_sem=o_ssem.at[step], recv_sem=o_rsem.at[step],
            device_id={"yax": y_to, "xax": lax.rem(other, x_size)}, device_id_type=MESH)

    def over_tiles(body, low=0, high=None):
        high = full_tiles + 1 if high is None else high

        @pl.loop(low, min(high, full_tiles))
        def _(tile):
            body(tile, V_TILE)
        if high > full_tiles:
            body(full_tiles, tail)

    ins = [pltpu.make_async_copy(keep_ref.at[pl.ds(0, half), :], gu_keep.at[0], in_sem.at[0]),
           pltpu.make_async_copy(got_a_ref, gu_got.at[0], in_sem.at[1]),
           pltpu.make_async_copy(w_out_ref, w_out, in_sem.at[2]),
           pltpu.make_async_copy(w_down_ref, w_down, in_sem.at[3]),
           pltpu.make_async_copy(keep_ref.at[pl.ds(half, half), :], gu_keep.at[1], in_sem.at[4]),
           pltpu.make_async_copy(got_b_ref, gu_got.at[1], in_sem.at[5])]
    for item in ins:
        item.start()
    all_barrier(y_size, x_size, y_idx, d_idx)

    def front_m(chunk):
        gated = gu_keep[chunk] + gu_got[chunk]
        gate = gated[:, :ff_cols].astype(jnp.bfloat16).astype(jnp.float32)
        up_val = gated[:, ff_cols:].astype(jnp.bfloat16).astype(jnp.float32)
        m_all[chunk, d_idx] = (gate * (1.0 / (1.0 + jnp.exp(-gate))) * up_val).astype(jnp.bfloat16)
        m_copy(chunk, 1).start()
        m_copy(chunk, 0).start()

    def front_rest(chunk):
        span = pl.ds(chunk * half, half)

        def down(slot):
            return jnp.dot(m_all[chunk, slot], w_down[pl.ds(pl.multiple_of(slot * ff_cols, ff_cols), ff_cols), :],
                           preferred_element_type=jnp.float32)
        sum_own[chunk] = jnp.dot(o_all[span, :], w_out[...], preferred_element_type=jnp.float32) + down(d_idx)
        m_copy(chunk, 0).wait_recv()
        sum_own[chunk] += down(partner)
        m_copy(chunk, 1).wait_recv()
        m_copy(chunk, 2).start()
        sum_own[chunk] += down(x_nbr)
        m_copy(chunk, 2).wait_recv()
        sum_own[chunk] += down(x_diag)
        sum_copy(chunk).start()
        sum_copy(chunk).wait_recv()
        res = hid_ref[span, :].astype(jnp.float32) + (sum_own[chunk] + sum_peer[chunk])
        packed = compact_rows(*local_moments(res))
        mom_own[chunk] = packed
        mom_all[chunk, d_idx] = packed
        for step in range(1, x_size):
            mom_copy(chunk, step).start()
        for step in range(1, x_size):
            mom_copy(chunk, step).wait_recv()
        mean, rstd = spread_rows(*join_moments([mom_all[chunk, i] for i in range(x_size)], x_size, part))
        f_own[chunk] = ((res - mean) * rstd * gain_ref[0:1, :]).astype(jnp.bfloat16)
        f_copy(chunk).start()

    def partial(chunk, quarter, tile, size):
        off = pl.multiple_of(tile * V_TILE, V_TILE)
        return (lax.dot_general(ebuf[0, quarter, pl.ds(off, size), :], f_own[chunk], NT_DIMS,
                                preferred_element_type=jnp.float32)
                + lax.dot_general(ebuf[1, quarter, pl.ds(off, size), :], f_peer[chunk], NT_DIMS,
                                  preferred_element_type=jnp.float32))

    def send_tiles(chunk, low, high):
        def one(tile, size):
            if chunk == 0:
                e_own_copy(0, tile, size).wait()
                e_peer_copy(0, tile, size).wait_recv()
            off = pl.multiple_of(tile * V_TILE, V_TILE)
            send[chunk, pl.ds(off, size), :] = partial(chunk, 0, tile, size)

        @pl.loop(low, min(high, full_tiles))
        def _(tile):
            one(tile, V_TILE)

            @pl.when(tile > low)
            def _():
                z_copy(chunk, tile - 1, V_TILE).start()
        if high > full_tiles:
            one(full_tiles, tail)
            z_copy(chunk, full_tiles - 1, V_TILE).start()
            z_copy(chunk, full_tiles, tail).start()
        else:
            z_copy(chunk, high - 1, V_TILE).start()

    def out_copy(chunk, tile, size):
        span = pl.ds(pl.multiple_of(tile * V_TILE, V_TILE), size)
        return pltpu.make_async_copy(recv.at[chunk, span, :], z_ref.at[span, pl.ds(chunk * half, half)],
                                     out_sem.at[chunk, tile])

    def take_tile(chunk, tile, size, carry):
        run_max, run_sum = carry
        off = pl.multiple_of(tile * V_TILE, V_TILE)
        if chunk == 0:
            e_own_copy(1, tile, size).wait()
            e_peer_copy(1, tile, size).wait_recv()
        own = partial(chunk, 1, tile, size)
        z_copy(chunk, tile, size).wait_recv()
        z_val = own + recv[chunk, pl.ds(off, size), :]
        recv[chunk, pl.ds(off, size), :] = z_val
        z_grp = z_val.reshape(size // 8, 8, half)
        new_max = jnp.maximum(run_max, jnp.max(z_grp, axis=0))
        new_sum = run_sum * jnp.exp(run_max - new_max) + jnp.sum(jnp.exp(z_grp - new_max[None]), axis=0)
        out_copy(chunk, tile, size).start()
        return new_max, new_sum

    def stat_copy(chunk, step):
        other = lax.rem(flat + step, n_dev)
        return pltpu.make_async_remote_copy(
            src_ref=stat_own.at[chunk], dst_ref=stat_all.at[chunk, flat], send_sem=stat_ssem.at[chunk, step],
            recv_sem=stat_rsem.at[chunk, step],
            device_id={"yax": other // x_size, "xax": lax.rem(other, x_size)}, device_id_type=MESH)

    def gather_chunk(chunk):
        low = jnp.full((8, half), -jnp.inf, jnp.float32)
        carry = take_tile(chunk, 0, V_TILE, (low, jnp.zeros((8, half), jnp.float32)))
        carry = lax.fori_loop(1, full_tiles, lambda tile, c: take_tile(chunk, tile, V_TILE, c), carry)
        run_max, run_sum = take_tile(chunk, full_tiles, tail, carry)
        top = jnp.max(run_max, axis=0, keepdims=True)
        total = jnp.sum(run_sum * jnp.exp(run_max - top), axis=0, keepdims=True)
        sub = lax.broadcasted_iota(jnp.int32, (8, half), 0)
        both = jnp.where(sub == 0, top, total)
        stat_own[chunk] = both
        stat_all[chunk, flat] = both
        for step in range(1, n_dev):
            stat_copy(chunk, step).start()

    def norm_chunk(chunk):
        for step in range(1, n_dev):
            stat_copy(chunk, step).wait_recv()
        tops = [stat_all[chunk, i, 0:1, :] for i in range(n_dev)]
        top_all = tops[0]
        for item in tops[1:]:
            top_all = jnp.maximum(top_all, item)
        sum_all = jnp.zeros_like(top_all)
        for i in range(n_dev):
            sum_all = sum_all + stat_all[chunk, i, 1:2, :] * jnp.exp(tops[i] - top_all)
        norm_ref[:, pl.ds(chunk * half, half)] = top_all + jnp.log(sum_all)

    ins[0].wait()
    ins[1].wait()
    front_m(0)
    for step in range(1, n_dev):
        o_copy(step).start()
    over_tiles(lambda tile, size: e_own_copy(0, tile, size).start())
    over_tiles(lambda tile, size: e_peer_copy(0, tile, size).start())
    over_tiles(lambda tile, size: e_own_copy(1, tile, size).start())
    over_tiles(lambda tile, size: e_peer_copy(1, tile, size).start())
    o_all[pl.ds(pl.multiple_of(flat * own_rows, own_rows), own_rows), :] = att_ref[
        :, pl.ds(pl.multiple_of(y_idx * o_cols, 128), o_cols)]
    ins[2].wait()
    ins[3].wait()
    for step in range(1, n_dev):
        o_copy(step).wait_recv()
    front_rest(0)
    f_copy(0).wait_recv()
    split = full_tiles // 2
    send_tiles(0, 0, split)
    ins[4].wait()
    ins[5].wait()
    front_m(1)
    send_tiles(0, split, full_tiles + 1)
    front_rest(1)
    f_copy(1).wait_recv()
    send_tiles(1, 0, full_tiles + 1)
    for chunk in range(chunks):
        gather_chunk(chunk)
    for chunk in range(chunks):
        norm_chunk(chunk)

    for step in range(1, n_dev):
        o_copy(step).wait_send()
    for chunk in range(chunks):
        f_copy(chunk).wait_send()
        sum_copy(chunk).wait_send()
        for which in range(3):
            m_copy(chunk, which).wait_send()
        for step in range(1, x_size):
            mom_copy(chunk, step).wait_send()
        for step in range(1, n_dev):
            stat_copy(chunk, step).wait_send()
        over_tiles(lambda tile, size: z_copy(chunk, tile, size).wait_send())
        over_tiles(lambda tile, size: e_peer_copy(chunk, tile, size).wait_send())
        over_tiles(lambda tile, size: out_copy(chunk, tile, size).wait())


def head_call(mesh, attn_own, hidden, gain, keep, got_a, got_b, w_out, w_down, embedding):
    y_size, x_size = mesh.shape["yax"], mesh.shape["xax"]
    rows, part = hidden.shape
    v_quarter = embedding.shape[0] // x_size
    half = rows // 2
    tiles = v_quarter // V_TILE + 1
    n_dev = y_size * x_size
    o_cols = w_out.shape[0]
    ff_cols = w_down.shape[0] // x_size
    dma, vm, f32, bf16 = pltpu.SemaphoreType.DMA, pltpu.VMEM, jnp.float32, jnp.bfloat16
    any_spec = pl.BlockSpec(memory_space=pl.ANY)
    vmem_spec = pl.BlockSpec(memory_space=pltpu.VMEM)
    return pl.pallas_call(
        functools.partial(head_kernel, y_size, x_size),
        out_shape=(jax.ShapeDtypeStruct((v_quarter, rows), f32), jax.ShapeDtypeStruct((1, rows), f32)),
        in_specs=[vmem_spec] * 3 + [any_spec] * 6,
        out_specs=(any_spec, vmem_spec),
        scratch_shapes=[
            vm((2, 2, v_quarter, part), bf16), vm((2, half, part), bf16), vm((2, half, part), bf16),
            vm((2, v_quarter, half), f32), vm((2, v_quarter, half), f32),
            vm((rows, o_cols), bf16), vm((2, x_size, half, ff_cols), bf16), vm(w_out.shape, bf16), vm(w_down.shape, bf16),
            vm((2, half, 2 * ff_cols), f32), vm((2, half, 2 * ff_cols), f32),
            vm((2, half, part), f32), vm((2, half, part), f32),
            vm((2, 8, half), f32), vm((2, x_size, 8, half), f32), vm((2, 8, half), f32), vm((2, n_dev, 8, half), f32),
            dma((2, tiles)), dma((2, tiles)), dma((2, tiles)), dma((2,)), dma((2,)), dma((2, tiles)), dma((2, tiles)),
            dma((2, n_dev)), dma((2, n_dev)), dma((2, tiles)),
            dma((n_dev,)), dma((n_dev,)), dma((2, 3)), dma((2, 3)), dma((6,)), dma((2,)), dma((2,)),
            dma((2, x_size)), dma((2, x_size))],
        compiler_params=pltpu.CompilerParams(collective_id=0, has_side_effects=True,
                                             vmem_limit_bytes=63 * 1024 * 1024),
        cost_estimate=pl.CostEstimate(flops=2 * rows * 2 * v_quarter * 2 * part, bytes_accessed=40_000_000,
                                      transcendentals=rows * v_quarter),
        name="head",
    )(attn_own, hidden, gain[None, :], keep, got_a, got_b, w_out, w_down, embedding)


def solution(mesh):
    y_size = mesh.shape["yax"]
    x_size = mesh.shape["xax"]
    row_spec = P(("dp", "yax", "xax"))

    def local_step(hidden, cache_len, k_cache, v_cache, g_attn, w_query, w_key, w_value,
                   w_gate, w_up, w_out, w_down, g_final, embedding):
        rows = hidden.shape[0]
        own_rows = k_cache.shape[0]
        head_dim = k_cache.shape[2]
        heads = y_size * w_query.shape[1] // head_dim
        own_start = (lax.axis_index("yax") * x_size + lax.axis_index("xax")) * own_rows
        len_own = lax.dynamic_slice_in_dim(cache_len, own_start, own_rows, axis=0)
        angles = rope_angle(len_own, head_dim)
        cos_a, sin_a = jnp.cos(angles), jnp.sin(angles)
        cos_a = jnp.concatenate([cos_a, cos_a], axis=1)
        sin_a = jnp.concatenate([-sin_a, sin_a], axis=1)
        query, key_own, value_own, keep, send_a, send_b = project_call(
            mesh, hidden, g_attn, cos_a, sin_a, w_query, w_key, w_value, w_gate, w_up)
        across = [(i, (i + x_size // 2) % x_size) for i in range(x_size)]
        got_a = lax.ppermute(send_a, "xax", across)
        got_b = lax.ppermute(send_b, "xax", across)
        attn_own, key_own, value_own = attend_call(query.reshape(own_rows, heads, head_dim), k_cache, v_cache, key_own, value_own, len_own)
        z_val, log_norm = head_call(mesh, attn_own.reshape(own_rows, heads * head_dim), hidden, g_final, keep, got_a,
                                    got_b, w_out, w_down, embedding)
        return key_own, value_own, (z_val - log_norm).T, log_norm.reshape(rows)

    in_specs = (P("dp", "xax"), P("dp"), row_spec, row_spec, P("xax"), P("xax", "yax"),
                P("xax", None), P("xax", None), P("xax", "yax"), P("xax", "yax"),
                P("yax", "xax"), P("yax", "xax"), P("xax"), P("yax", "xax"))
    out_specs = (row_spec, row_spec, P("dp", ("yax", "xax")), P("dp"))
    return jax.shard_map(local_step, mesh=mesh, in_specs=in_specs, out_specs=out_specs, check_vma=False)
```
